128 devices in a mesh: dp: 16 (over z, y), pp: 8 (over x, core).
Axes of the slice: x: 4, y: 4, z: 4, core: 2. Of those that a mesh axis runs over, the one named last changes fastest.
Arguments:
- tok_ids: int32 [1, 16, 130], P(None, 'dp')
- emb_s: bfloat16 [8, 50304, 1024], P('pp', 'dp')
- w_one: bfloat16 [8, 1, 1024, 4096], P('pp')
- w_two: bfloat16 [8, 1, 4096, 1024], P('pp')
- gain_f: bfloat16 [1024], replicated
- gain_h: bfloat16 [1024], replicated
- gain_e: bfloat16 [1024], replicated
- gain_m: bfloat16 [1024], replicated
- w_proj: bfloat16 [2048, 1024], replicated
- u_one: bfloat16 [1024, 4096], replicated
- u_two: bfloat16 [4096, 1024], replicated
- w_out: bfloat16 [1024, 50304], replicated
Outputs:
- output 1: float32 [], replicated
- output 2: float32 [1, 16, 128], P(None, 'dp')
- output 3: float32 [1, 16, 128], P(None, 'dp')
All inputs are finite; a program needn't handle non-finite values.
Results may differ from the reference program's by a relative error of at most 0.00387627.
Values are sent between devices in bfloat16 or wider.
A program may use at most 1 GiB of HBM per device.

```python
import jax
import jax.numpy as jnp
from jax import lax

STAGES = 8
LAYERS = 1
MICRO_BATCHES = 1
GLOBAL_BATCH = 16
SEQ_LEN = 128
HIDDEN = 1024
FFN_HIDDEN = 4096
VOCAB_SIZE = 50304
HEAD_ROWS = 128
NORM_EPS = 1e-6
MTP_WEIGHT = 0.3


def setup_inputs(seed: int = 0) -> dict:
    key_list = jax.random.split(jax.random.key(seed), 12)
    tok_ids = jax.random.randint(key_list[0], (MICRO_BATCHES, GLOBAL_BATCH, SEQ_LEN + 2), 0, VOCAB_SIZE, dtype=jnp.int32)
    tok_ids = tok_ids.at[0, 0, 0].set(0).at[0, 0, 1].set(VOCAB_SIZE - 1)
    table = jax.random.normal(key_list[1], (VOCAB_SIZE, HIDDEN), jnp.float32).astype(jnp.bfloat16)
    emb_s = jnp.concatenate([table[None], jnp.zeros((STAGES - 1, VOCAB_SIZE, HIDDEN), jnp.bfloat16)], axis=0)
    w_one = (jax.random.normal(key_list[2], (STAGES, LAYERS, HIDDEN, FFN_HIDDEN), jnp.float32) * HIDDEN ** -0.5).astype(jnp.bfloat16)
    w_two = (jax.random.normal(key_list[3], (STAGES, LAYERS, FFN_HIDDEN, HIDDEN), jnp.float32) * FFN_HIDDEN ** -0.5).astype(jnp.bfloat16)
    gain_f = jax.random.uniform(key_list[4], (HIDDEN,), jnp.float32, 0.25, 1.75).astype(jnp.bfloat16)
    gain_h = jax.random.uniform(key_list[5], (HIDDEN,), jnp.float32, 0.25, 1.75).astype(jnp.bfloat16)
    gain_e = jax.random.uniform(key_list[6], (HIDDEN,), jnp.float32, 0.25, 1.75).astype(jnp.bfloat16)
    gain_m = jax.random.uniform(key_list[7], (HIDDEN,), jnp.float32, 0.25, 1.75).astype(jnp.bfloat16)
    w_proj = (jax.random.normal(key_list[8], (2 * HIDDEN, HIDDEN), jnp.float32) * (2 * HIDDEN) ** -0.5).astype(jnp.bfloat16)
    u_one = (jax.random.normal(key_list[9], (HIDDEN, FFN_HIDDEN), jnp.float32) * HIDDEN ** -0.5).astype(jnp.bfloat16)
    u_two = (jax.random.normal(key_list[10], (FFN_HIDDEN, HIDDEN), jnp.float32) * FFN_HIDDEN ** -0.5).astype(jnp.bfloat16)
    w_out = (jax.random.normal(key_list[11], (HIDDEN, VOCAB_SIZE), jnp.float32) * 3.0 * HIDDEN ** -0.5).astype(jnp.bfloat16)
    return {'tok_ids': tok_ids, 'emb_s': emb_s, 'w_one': w_one, 'w_two': w_two, 'gain_f': gain_f, 'gain_h': gain_h, 'gain_e': gain_e, 'gain_m': gain_m, 'w_proj': w_proj, 'u_one': u_one, 'u_two': u_two, 'w_out': w_out}


def norm_plain(x_val):
    x_f = x_val.astype(jnp.float32)
    return (x_f * lax.rsqrt(jnp.mean(x_f * x_f, axis=-1, keepdims=True) + NORM_EPS)).astype(jnp.bfloat16)


def norm_gain(x_val, gain_vec):
    x_f = x_val.astype(jnp.float32)
    scaled = x_f * lax.rsqrt(jnp.mean(x_f * x_f, axis=-1, keepdims=True) + NORM_EPS)
    return (scaled * gain_vec.astype(jnp.float32)).astype(jnp.bfloat16)


def mlp_add(x_val, normed, w_up, w_down):
    hidden = jax.nn.gelu(jnp.dot(normed, w_up, preferred_element_type=jnp.float32)).astype(jnp.bfloat16)
    return (x_val.astype(jnp.float32) + jnp.dot(hidden, w_down, preferred_element_type=jnp.float32)).astype(jnp.bfloat16)


def row_nll(normed, targets, w_out):
    n_blocks = normed.shape[0] // HEAD_ROWS

    def one_block(pair):
        block_rows, block_tgt = pair
        logits = jnp.dot(block_rows, w_out, preferred_element_type=jnp.float32)
        picked = jnp.take_along_axis(logits, block_tgt[:, None], axis=1)[:, 0]
        return jax.nn.logsumexp(logits, axis=1) - picked

    per_block = lax.map(one_block, (normed.reshape(n_blocks, HEAD_ROWS, HIDDEN), targets.reshape(n_blocks, HEAD_ROWS)))
    return per_block.reshape(n_blocks * HEAD_ROWS)


def reference(tok_ids, emb_s, w_one, w_two, gain_f, gain_h, gain_e, gain_m, w_proj, u_one, u_two, w_out):
    table = emb_s[0]
    w_up = w_one.reshape(STAGES * LAYERS, HIDDEN, FFN_HIDDEN)
    w_down = w_two.reshape(STAGES * LAYERS, FFN_HIDDEN, HIDDEN)
    seqs = tok_ids.reshape(MICRO_BATCHES * GLOBAL_BATCH, SEQ_LEN + 2)

    def layer_step(x_val, weights):
        w_a, w_b = weights
        return mlp_add(x_val, norm_plain(x_val), w_a, w_b), None

    def per_sequence(ids):
        x_val = table[ids[:SEQ_LEN]]
        h_last, _ = lax.scan(layer_step, x_val, (w_up, w_down))
        main_nll = row_nll(norm_gain(h_last, gain_f), ids[1:SEQ_LEN + 1], w_out)
        e_rows = table[ids[1:SEQ_LEN + 1]]
        joined = jnp.concatenate([norm_gain(h_last, gain_h), norm_gain(e_rows, gain_e)], axis=1)
        z_val = jnp.dot(joined, w_proj, preferred_element_type=jnp.float32).astype(jnp.bfloat16)
        z_val = mlp_add(z_val, norm_gain(z_val, gain_m), u_one, u_two)
        mtp_nll = row_nll(norm_gain(z_val, gain_f), ids[2:], w_out)
        return main_nll, mtp_nll

    main_nll, mtp_nll = lax.map(per_sequence, seqs)
    main_nll = main_nll.reshape(MICRO_BATCHES, GLOBAL_BATCH, SEQ_LEN)
    mtp_nll = mtp_nll.reshape(MICRO_BATCHES, GLOBAL_BATCH, SEQ_LEN)
    total_loss = jnp.mean(main_nll) + MTP_WEIGHT * jnp.mean(mtp_nll)
    return (total_loss, main_nll, mtp_nll)
```

```python
import functools

import jax
import jax.numpy as jnp
from jax import lax
from jax.experimental import pallas as pl
from jax.experimental.pallas import tpu as pltpu
from jax.sharding import PartitionSpec as P

NORM_EPS = 1e-6
MTP_WEIGHT = 0.3
HEAD_ROWS = 128
LANES = 128
SUB = 8
ID_PAD = 256
CAP = 24
PIECE = 256
MLP_BLOCK = 1024
VMEM_LIMIT = 66_900_000
F32 = jnp.float32
BF16 = jnp.bfloat16
MESH = pl.DeviceIdType.MESH


def norm_f32(x_f):
    return x_f * lax.rsqrt(jnp.mean(x_f * x_f, axis=-1, keepdims=True) + NORM_EPS)


def iota(shape, dim):
    return lax.broadcasted_iota(jnp.int32, shape, dim)


def dot32(a, b):
    return jnp.dot(a, b, preferred_element_type=F32)


def mega_kernel(
    n_dp, n_pp, seq, cap,
    ids_ref, gains_ref, emb, w1h, w2h, wph, u1h, u2h, woh,
    main_out, mtp_out, loss_out, flag_out,
    w1, w2, u1, u2, wp, wo,
    ids_all, send_rows, recv_rows, xbuf, ybuf, xnb, hid, ebuf, hbuf, eall, zbuf, epart, xh, lg, mx, sm, pk,
    part_send, part_recv, ls_send, ls_recv,
    wsem, ids_ss, ids_rs, row_ss, row_rs, x_ss, x_rs, e_ss, e_rs, h_ss, h_rs, f_ss, part_ss, part_rs, ls_ss, ls_rs,
):
    d = lax.axis_index("dp")
    p = lax.axis_index("pp")
    width = xbuf.shape[1]
    ffn = w1.shape[1]
    n_rows = emb.shape[1]
    half = seq // 2
    n_shard = n_pp // 2
    shard = lax.rem(p, n_shard)
    group = p // n_shard
    n_tiles = woh.shape[1] // LANES
    base_tiles = n_tiles // n_shard
    cols = w1.shape[1] + wo.shape[1]
    own_cols = wo.shape[1]
    n_piece = width // PIECE
    is_first = p == 0
    is_last = p == n_pp - 1
    k_main = n_rows // ID_PAD * ID_PAD
    k_pad = k_main + ID_PAD

    col0 = pl.multiple_of(shard * (base_tiles * LANES), LANES)
    tab_cp = pltpu.make_async_copy(emb.at[0], u2.at[pl.ds(0, n_rows), :], wsem.at[0])
    w1_cp = pltpu.make_async_copy(w1h.at[0, 0], w1, wsem.at[1])
    w2_cp = pltpu.make_async_copy(w2h.at[0, 0], w2, wsem.at[2])
    u1_cp = pltpu.make_async_copy(u1h, u1, wsem.at[3])
    u2_cp = pltpu.make_async_copy(u2h, u2, wsem.at[4])
    wp_cp = pltpu.make_async_copy(wph, wp, wsem.at[5])
    wo_cp = pltpu.make_async_copy(woh.at[:, pl.ds(col0 + ffn, own_cols)], wo, wsem.at[6])
    late_cp = pltpu.make_async_copy(woh.at[:, pl.ds(col0, ffn)], w1, wsem.at[7])

    @pl.when(is_first)
    def _():
        tab_cp.start()

    @pl.when(jnp.logical_not(is_first))
    def _():
        w1_cp.start()
        w2_cp.start()

    barrier = pltpu.get_barrier_semaphore()
    for k in range(1, n_dp):
        pl.semaphore_signal(barrier, inc=1, device_id={"dp": lax.rem(d + k, n_dp)}, device_id_type=MESH)
    for k in range(1, n_pp):
        pl.semaphore_signal(barrier, inc=1, device_id={"pp": lax.rem(p + k, n_pp)}, device_id_type=MESH)
    pl.semaphore_wait(barrier, n_dp - 1 + n_pp - 1)

    def ids_copy(owner, peer):
        return pltpu.make_async_remote_copy(
            src_ref=ids_ref, dst_ref=ids_all.at[owner], send_sem=ids_ss.at[peer], recv_sem=ids_rs.at[owner],
            device_id={"dp": peer}, device_id_type=MESH)

    for k in range(1, n_dp):
        ids_copy(d, lax.rem(d + k, n_dp)).start()
    ids_all[d] = ids_ref[...]

    @pl.when(jnp.logical_not(is_first))
    def _():
        u1_cp.start()
        u2_cp.start()
        wp_cp.start()
        wo_cp.start()

    for k in range(1, n_dp):
        peer = lax.rem(d + k, n_dp)
        ids_copy(peer, peer).wait_recv()

    def set_flag():
        ids2 = ids_all[...].reshape(n_dp * SUB, ID_PAD)
        used = iota((n_dp * SUB, ID_PAD), 1) < seq + 1
        most = jnp.zeros((n_dp * SUB, 1), F32)
        for k in range(n_dp):
            hit = (ids2 >= k * n_rows) & (ids2 < (k + 1) * n_rows) & used
            most = jnp.maximum(most, jnp.sum(jnp.where(hit, 1.0, 0.0), axis=1, keepdims=True))
        over = jnp.max(most, axis=0, keepdims=True)
        flag_out[...] = jnp.broadcast_to(jnp.where(over > cap, 1.0, 0.0), (SUB, LANES))

    def row_copy(owner, peer):
        return pltpu.make_async_remote_copy(
            src_ref=send_rows.at[peer], dst_ref=recv_rows.at[owner], send_sem=row_ss.at[peer], recv_sem=row_rs.at[owner],
            device_id={"dp": peer}, device_id_type=MESH)

    @pl.when(is_first)
    def _():
        w1_cp.start()
        w2_cp.start()
        low = d * n_rows
        ids2 = ids_all[...].reshape(n_dp * SUB, ID_PAD)
        lane2 = iota((n_dp * SUB, ID_PAD), 1)
        valid = (ids2 >= low) & (ids2 < low + n_rows) & (lane2 < seq + 1)
        before = jnp.where(iota((ID_PAD, ID_PAD), 0) < iota((ID_PAD, ID_PAD), 1), 1.0, 0.0).astype(BF16)
        rank = dot32(jnp.where(valid, 1.0, 0.0).astype(BF16), before)
        key = jnp.where(valid, rank, -1.0)
        loc = jnp.where(valid, ids2 - low, 0).astype(F32)
        slot = iota((cap, ID_PAD), 0).astype(F32)
        for b in range(0, n_dp, 2):
            picks = []
            for s in (b, b + 1):
                sel = key[s * SUB:s * SUB + 1, :] == slot
                idx = jnp.sum(jnp.where(sel, loc[s * SUB:s * SUB + 1, :] + 1.0, 0.0), axis=1, keepdims=True) - 1.0
                picks.append(idx)
            idx2 = jnp.concatenate(picks, axis=0).astype(jnp.int32)
            hot = jnp.where(iota((2 * cap, k_pad), 1) == idx2, 1.0, 0.0).astype(BF16)
            u1[b * cap:(b + 2) * cap, 0:k_pad] = hot
        tab_cp.wait()
        n_slots = n_dp * cap
        blk = min(512, width)
        for c in range(0, width, blk):
            tail = u2[k_main:k_pad, c:c + blk]
            tail = jnp.where(iota((ID_PAD, blk), 0) < n_rows - k_main, tail.astype(F32), 0.0).astype(BF16)
            got = dot32(u1[0:n_slots, 0:k_main], u2[0:k_main, c:c + blk]) + dot32(u1[0:n_slots, k_main:k_pad], tail)
            for s in range(n_dp):
                send_rows[s, :, c:c + blk] = got[s * cap:(s + 1) * cap, :].astype(BF16)
        for k in range(1, n_dp):
            row_copy(d, lax.rem(d + k, n_dp)).start()
        recv_rows[d] = send_rows[d]
        u1_cp.start()
        u2_cp.start()
        wp_cp.start()
        wo_cp.start()
        row = ids_ref[0:1, :]
        rr = iota((2 * seq, ID_PAD), 0)
        ll = iota((2 * seq, ID_PAD), 1)
        pos = jnp.where(rr < seq, rr, rr - seq + 1)
        id_col = jnp.sum(jnp.where(ll == pos, jnp.broadcast_to(row, (2 * seq, ID_PAD)), 0).astype(F32), axis=1, keepdims=True)
        src_col = jnp.zeros((2 * seq, 1), F32)
        src_row = jnp.zeros((1, ID_PAD), F32)
        for k in range(1, n_dp):
            src_col = src_col + jnp.where(id_col >= float(k * n_rows), 1.0, 0.0)
            src_row = src_row + jnp.where(row >= k * n_rows, 1.0, 0.0)
        earlier = (jnp.broadcast_to(src_row, (2 * seq, ID_PAD)) == src_col) & (ll < pos)
        rank_col = jnp.sum(jnp.where(earlier, 1.0, 0.0), axis=1, keepdims=True)
        where_col = jnp.where(rank_col < float(cap), src_col * float(cap) + rank_col, -1.0).astype(jnp.int32)
        place = jnp.where(iota((2 * seq, n_slots), 1) == where_col, 1.0, 0.0).astype(BF16)
        for k in range(1, n_dp):
            peer = lax.rem(d + k, n_dp)
            row_copy(peer, peer).wait_recv()
        rows = dot32(place, recv_rows[...].reshape(n_slots, width)).astype(BF16)
        xbuf[...] = rows[0:seq, :]
        eall[...] = rows[seq:2 * seq, :]

    @pl.when(jnp.logical_not(is_first))
    def _():
        set_flag()

    def x_copy(i):
        part = pl.ds(i * PIECE, PIECE)
        return pltpu.make_async_remote_copy(
            src_ref=ybuf.at[:, part], dst_ref=xbuf.at[:, part], send_sem=x_ss.at[i], recv_sem=x_rs.at[i],
            device_id={"pp": lax.rem(p + 1, n_pp)}, device_id_type=MESH)

    h_peers = ((1, 0), (3, 0), (5, half), (6, half))

    def h_copy(j, i):
        to, row0 = h_peers[j]
        part = pl.ds(i * PIECE, PIECE)
        return pltpu.make_async_remote_copy(
            src_ref=ybuf.at[pl.ds(row0, half), part], dst_ref=hbuf.at[:, part], send_sem=h_ss.at[j, i], recv_sem=h_rs.at[i],
            device_id={"pp": to}, device_id_type=MESH)

    def f_copy(i):
        part = pl.ds(i * PIECE, PIECE)
        return pltpu.make_async_remote_copy(
            src_ref=hbuf.at[:, part], dst_ref=hbuf.at[:, part], send_sem=f_ss.at[i], recv_sem=h_rs.at[i],
            device_id={"pp": lax.rem(p + n_pp - 1, n_pp)}, device_id_type=MESH)

    def gelu_up(m, xn, w_up):
        for c in range(0, ffn, MLP_BLOCK):
            hid[0:m, c:c + MLP_BLOCK] = jax.nn.gelu(dot32(xn, w_up[:, c:c + MLP_BLOCK])).astype(BF16)

    w1_cp.wait()

    @pl.when(jnp.logical_not(is_first))
    def _():
        for i in range(n_piece):
            x_copy(i).wait_recv()

    xnb[...] = norm_f32(xbuf[...].astype(F32)).astype(BF16)
    gelu_up(seq, xnb[...], w1)
    w2_cp.wait()
    for i in range(n_piece):
        c = i * PIECE
        out = xbuf[:, c:c + PIECE].astype(F32) + dot32(hid[...], w2[:, c:c + PIECE])
        ybuf[:, c:c + PIECE] = out.astype(BF16)

        @pl.when(jnp.logical_not(is_last))
        def _():
            x_copy(i).start()

        @pl.when(is_last)
        def _():
            for j in range(len(h_peers)):
                h_copy(j, i).start()

    late_cp.start()

    def e_copy(to):
        row0 = half * (to // n_shard)
        return pltpu.make_async_remote_copy(
            src_ref=eall.at[pl.ds(row0, half), :], dst_ref=ebuf, send_sem=e_ss.at[to], recv_sem=e_rs,
            device_id={"pp": to}, device_id_type=MESH)

    @pl.when(is_first)
    def _():
        for to in range(1, n_pp):
            e_copy(to).start()
        ebuf[...] = eall[0:half, :]
        set_flag()

    @pl.when(jnp.logical_not(is_first))
    def _():
        e_copy(1).wait_recv()

    g_f = gains_ref[0:1, :]
    g_h = gains_ref[1:2, :]
    g_e = gains_ref[2:3, :]
    g_m = gains_ref[3:4, :]

    wp_cp.wait()
    e_n = (norm_f32(ebuf[...].astype(F32)) * g_e).astype(BF16)
    epart[...] = dot32(e_n, wp[width:2 * width, :])
    u1_cp.wait()
    u2_cp.wait()
    wo_cp.wait()

    row_f = jnp.broadcast_to(ids_ref[0:1, :], (2 * half, ID_PAD))
    rr = iota((2 * half, ID_PAD), 0)
    at = jnp.where(rr < half, rr + 1, rr - half + 2) + group * half
    tgt = jnp.sum(jnp.where(iota((2 * half, ID_PAD), 1) == at, row_f, 0).astype(F32), axis=1, keepdims=True)
    tgt = tgt.astype(jnp.int32) - shard * (base_tiles * LANES)
    tgt = jnp.broadcast_to(tgt, (2 * half, LANES))

    @pl.when(is_last)
    def _():
        hbuf[...] = ybuf[half:seq, :]

    @pl.when(jnp.logical_not(is_last))
    def _():
        for i in range(n_piece):
            h_copy(0, i).wait_recv()

            @pl.when((p == 1) | (p == 3) | (p == 5))
            def _():
                f_copy(i).start()

    h_f = norm_f32(hbuf[...].astype(F32))
    z_val = (dot32((h_f * g_h).astype(BF16), wp[0:width, :]) + epart[...]).astype(BF16)
    zbuf[...] = z_val
    xh[0:half, :] = (h_f * g_f).astype(BF16)
    xnb[0:half, :] = (norm_f32(z_val.astype(F32)) * g_m).astype(BF16)
    gelu_up(half, xnb[0:half, :], u1)
    z_out = (zbuf[...].astype(F32) + dot32(hid[0:half, :], u2[...])).astype(BF16)
    xh[half:2 * half, :] = (norm_f32(z_out.astype(F32)) * g_f).astype(BF16)

    lane = iota((2 * half, LANES), 1)
    tail_ok = jnp.broadcast_to(shard == n_shard - 1, (2 * half, LANES))
    blocks = [(wo, c, ffn + c, min(MLP_BLOCK, own_cols - c)) for c in range(0, own_cols, MLP_BLOCK)]
    blocks += [(w1, c, c, MLP_BLOCK) for c in range(0, ffn, MLP_BLOCK)]

    def logits_of(i):
        ref, c, _, n = blocks[i]
        lg[i % 2, :, 0:n] = dot32(xh[...], ref[:, c:c + n])

    def fold(i):
        _, _, start, n = blocks[i]
        tiles = []
        for t in range(0, n, LANES):
            val = lg[i % 2, :, t:t + LANES]
            tiles.append((start + t, val, start + t == cols - LANES))
        top = None if i == 0 else mx[...]
        for _, val, last in tiles:
            val = jnp.where(tail_ok, val, -jnp.inf) if last else val
            top = val if top is None else jnp.maximum(top, val)
        total = jnp.zeros_like(top) if i == 0 else sm[...] * jnp.exp(mx[...] - top)
        hit = jnp.zeros_like(top) if i == 0 else pk[...]
        for at_col, val, last in tiles:
            e_val = jnp.exp(val - top)
            match = lane == tgt - at_col
            if last:
                e_val = jnp.where(tail_ok, e_val, 0.0)
                match = match & tail_ok
            total = total + e_val
            hit = hit + jnp.where(match, val, 0.0)
        mx[...] = top
        sm[...] = total
        pk[...] = hit

    for i in range(len(blocks)):
        if i == len(blocks) - ffn // MLP_BLOCK:
            late_cp.wait()
        logits_of(i)
        if i:
            fold(i - 1)
    fold(len(blocks) - 1)

    eye = iota((2 * half, LANES), 0) == iota((2 * half, LANES), 1)

    def as_row(col):
        return jnp.sum(jnp.where(eye, jnp.broadcast_to(col, (2 * half, LANES)), 0.0), axis=0, keepdims=True)

    top = mx[...]
    m_col = jnp.max(top, axis=1, keepdims=True)
    s_col = jnp.sum(sm[...] * jnp.exp(top - m_col), axis=1, keepdims=True)
    p_col = jnp.sum(pk[...], axis=1, keepdims=True)
    sub = iota((SUB, LANES), 0)
    tile = jnp.where(sub == 0, as_row(m_col), jnp.where(sub == 1, as_row(s_col), as_row(p_col)))
    part_send[...] = tile
    part_recv[p] = tile

    def part_copy(owner, peer):
        return pltpu.make_async_remote_copy(
            src_ref=part_send, dst_ref=part_recv.at[owner], send_sem=part_ss.at[peer], recv_sem=part_rs.at[owner],
            device_id={"pp": peer}, device_id_type=MESH)

    for k in range(1, n_pp):
        part_copy(p, lax.rem(p + k, n_pp)).start()
    for k in range(1, n_pp):
        peer = lax.rem(p + k, n_pp)
        part_copy(peer, peer).wait_recv()

    def group_nll(g):
        got = [part_recv[g * n_shard + i] for i in range(n_shard)]
        best = functools.reduce(jnp.maximum, [t[0:1, :] for t in got])
        total = sum(t[1:2, :] * jnp.exp(t[0:1, :] - best) for t in got)
        return best + jnp.log(total) - sum(t[2:3, :] for t in got)

    nll_a = jnp.broadcast_to(group_nll(0), (SUB, LANES))
    nll_b = jnp.broadcast_to(group_nll(1), (SUB, LANES))
    low_lane = iota((SUB, LANES), 1) < half
    main = jnp.where(low_lane, nll_a, pltpu.roll(nll_b, half, 1))
    mtp = jnp.where(low_lane, pltpu.roll(nll_a, half, 1), nll_b)
    main_out[...] = main[0:1, :]
    mtp_out[...] = mtp[0:1, :]
    both = main + MTP_WEIGHT * mtp
    ls_send[...] = both
    ls_recv[d] = both

    def ls_copy(owner, peer):
        return pltpu.make_async_remote_copy(
            src_ref=ls_send, dst_ref=ls_recv.at[owner], send_sem=ls_ss.at[peer], recv_sem=ls_rs.at[owner],
            device_id={"dp": peer}, device_id_type=MESH)

    for k in range(1, n_dp):
        ls_copy(d, lax.rem(d + k, n_dp)).start()
    for k in range(1, n_dp):
        peer = lax.rem(d + k, n_dp)
        ls_copy(peer, peer).wait_recv()
    acc = ls_recv[0]
    for k in range(1, n_dp):
        acc = acc + ls_recv[k]
    loss_out[...] = jnp.broadcast_to(jnp.sum(acc, axis=1, keepdims=True) * (1.0 / (n_dp * seq)), (SUB, LANES))

    for k in range(1, n_dp):
        peer = lax.rem(d + k, n_dp)
        ids_copy(d, peer).wait_send()
        ls_copy(d, peer).wait_send()
    for k in range(1, n_pp):
        part_copy(p, lax.rem(p + k, n_pp)).wait_send()

    @pl.when(is_first)
    def _():
        for k in range(1, n_dp):
            row_copy(d, lax.rem(d + k, n_dp)).wait_send()
        for to in range(1, n_pp):
            e_copy(to).wait_send()

    @pl.when(jnp.logical_not(is_last))
    def _():
        for i in range(n_piece):
            x_copy(i).wait_send()

    @pl.when((p == 1) | (p == 3) | (p == 5))
    def _():
        for i in range(n_piece):
            f_copy(i).wait_send()

    @pl.when(is_last)
    def _():
        for j in range(len(h_peers)):
            for i in range(n_piece):
                h_copy(j, i).wait_send()


def mega(n_dp, n_pp, seq, ids, gains, emb, w1, w2, wp, u1, u2, wo):
    width, ffn = w1.shape[2], w1.shape[3]
    n_tiles = wo.shape[1] // LANES
    n_shard = n_pp // 2
    cols = (n_tiles - (n_shard - 1) * (n_tiles // n_shard)) * LANES
    half = seq // 2
    n_piece = width // PIECE
    dma = pltpu.SemaphoreType.DMA
    tile = pltpu.VMEM((SUB, LANES), F32)
    vmem = pl.BlockSpec(memory_space=pltpu.VMEM)
    anys = pl.BlockSpec(memory_space=pl.ANY)
    act = pltpu.VMEM((seq, width), BF16)
    act_half = pltpu.VMEM((half, width), BF16)
    return pl.pallas_call(
        functools.partial(mega_kernel, n_dp, n_pp, seq, CAP),
        out_shape=(
            jax.ShapeDtypeStruct((1, seq), F32),
            jax.ShapeDtypeStruct((1, seq), F32),
            jax.ShapeDtypeStruct((SUB, LANES), F32),
            jax.ShapeDtypeStruct((SUB, LANES), F32),
        ),
        in_specs=[vmem] * 2 + [anys] * 7,
        out_specs=(vmem,) * 4,
        scratch_shapes=[
            pltpu.VMEM((width, ffn), BF16),
            pltpu.VMEM((ffn, width), BF16),
            pltpu.VMEM((width, ffn), BF16),
            pltpu.VMEM((ffn, width), BF16),
            pltpu.VMEM((2 * width, width), BF16),
            pltpu.VMEM((width, cols - ffn), BF16),
            pltpu.VMEM((n_dp, SUB, ID_PAD), jnp.int32),
            pltpu.VMEM((n_dp, CAP, width), BF16),
            pltpu.VMEM((n_dp, CAP, width), BF16),
            act, act, act,
            pltpu.VMEM((seq, ffn), BF16),
            act_half, act_half,
            act,
            act_half,
            pltpu.VMEM((half, width), F32),
            act,
            pltpu.VMEM((2, 2 * half, MLP_BLOCK), F32),
            pltpu.VMEM((2 * half, LANES), F32), pltpu.VMEM((2 * half, LANES), F32), pltpu.VMEM((2 * half, LANES), F32),
            tile, pltpu.VMEM((n_pp, SUB, LANES), F32),
            tile, pltpu.VMEM((n_dp, SUB, LANES), F32),
            dma((8,)), dma((n_dp,)), dma((n_dp,)), dma((n_dp,)), dma((n_dp,)),
            dma((n_piece,)), dma((n_piece,)), dma((n_pp,)), dma(()), dma((4, n_piece)), dma((n_piece,)), dma((n_piece,)),
            dma((n_pp,)), dma((n_pp,)), dma((n_dp,)), dma((n_dp,)),
        ],
        compiler_params=pltpu.CompilerParams(collective_id=0, has_side_effects=True, vmem_limit_bytes=VMEM_LIMIT),
        name="mtp_eval",
    )(ids, gains, emb, w1, w2, wp, u1, u2, wo)


def norm_plain(x_val):
    return norm_f32(x_val.astype(F32)).astype(BF16)


def norm_gain(x_val, gain_vec):
    return (norm_f32(x_val.astype(F32)) * gain_vec.astype(F32)).astype(BF16)


def mlp_add(x_val, normed, w_up, w_down):
    hidden = jax.nn.gelu(dot32(normed, w_up)).astype(BF16)
    return (x_val.astype(F32) + dot32(hidden, w_down)).astype(BF16)


def token_nll(normed, targets, w_out):
    n_rows, row_width = normed.shape
    n_blocks = n_rows // HEAD_ROWS

    def one_block(pair):
        block_rows, block_tgt = pair
        logits = dot32(block_rows, w_out)
        picked = jnp.take_along_axis(logits, block_tgt[:, None], axis=1)[:, 0]
        return jax.nn.logsumexp(logits, axis=1) - picked

    per_block = lax.map(one_block, (normed.reshape(n_blocks, HEAD_ROWS, row_width), targets.reshape(n_blocks, HEAD_ROWS)))
    return per_block.reshape(n_rows)


def any_ids(n_dp, n_pp, seq, ids, emb, w_one, w_two, gain_f, gain_h, gain_e, gain_m, w_proj, u_one, u_two, w_out):
    stage = lax.axis_index("pp")
    me = lax.axis_index("dp")
    n_rows, width = emb.shape
    ring = [(i, (i + 1) % n_dp) for i in range(n_dp)]
    want = ids[:seq + 1]

    def take(k, held, rows):
        local = want - lax.rem(me - k + n_dp, n_dp) * n_rows
        here = (local >= 0) & (local < n_rows)
        return jnp.where(here[:, None], held[jnp.clip(local, 0, n_rows - 1)], rows)

    def gather_step(k, carry):
        held, rows = carry
        rows = take(k, held, rows)
        return lax.ppermute(held, "dp", ring), rows

    rows = take(0, emb, jnp.zeros((seq + 1, width), BF16))
    _, rows = lax.fori_loop(1, n_dp, gather_step, (lax.ppermute(emb, "dp", ring), rows))
    to_next = [(i, i + 1) for i in range(n_pp - 1)]

    def tick(k, carry):
        x_val, _ = carry
        x_val = jnp.where((stage == 0) & (k == 0), rows[:seq], x_val)
        y_val = mlp_add(x_val, norm_plain(x_val), w_one, w_two)
        return lax.ppermute(y_val, "pp", to_next), y_val

    zero = jnp.zeros((seq, width), BF16)
    _, h_last = lax.fori_loop(0, n_pp, tick, (zero, zero))
    e_rows = lax.ppermute(rows[1:seq + 1], "pp", [(0, n_pp - 1)])
    main_nll = token_nll(norm_gain(h_last, gain_f), ids[1:seq + 1], w_out)
    z_sum = dot32(norm_gain(h_last, gain_h), w_proj[:width]) + dot32(norm_gain(e_rows, gain_e), w_proj[width:])
    z_val = z_sum.astype(BF16)
    z_val = mlp_add(z_val, norm_gain(z_val, gain_m), u_one, u_two)
    mtp_nll = token_nll(norm_gain(z_val, gain_f), ids[2:], w_out)
    is_last = stage == n_pp - 1
    main_nll = lax.psum(jnp.where(is_last, main_nll, 0.0), "pp")
    mtp_nll = lax.psum(jnp.where(is_last, mtp_nll, 0.0), "pp")
    total = lax.psum(jnp.sum(main_nll) + MTP_WEIGHT * jnp.sum(mtp_nll), "dp") / (n_dp * seq)
    return total, main_nll.reshape(1, seq), mtp_nll.reshape(1, seq)


def solution(mesh):
    n_pp = mesh.shape["pp"]
    n_dp = mesh.shape["dp"]

    def body(tok_ids, emb_s, w_one, w_two, gain_f, gain_h, gain_e, gain_m, w_proj, u_one, u_two, w_out):
        seq = tok_ids.shape[2] - 2
        ids = tok_ids.reshape(1, seq + 2)
        ids_pad = jnp.pad(jnp.broadcast_to(ids, (SUB, seq + 2)), ((0, 0), (0, ID_PAD - seq - 2)), constant_values=-1)
        gains = jnp.stack([gain_f, gain_h, gain_e, gain_m] * 2).astype(F32)
        main_nll, mtp_nll, total, over = mega(n_dp, n_pp, seq, ids_pad, gains, emb_s, w_one, w_two, w_proj, u_one, u_two, w_out)

        def slow():
            return any_ids(n_dp, n_pp, seq, ids[0], emb_s[0], w_one[0, 0], w_two[0, 0], gain_f, gain_h, gain_e, gain_m,
                           w_proj, u_one, u_two, w_out)

        def fast():
            return total[0, 0], main_nll, mtp_nll

        loss, main_nll, mtp_nll = lax.cond(over[0, 0] > 0.0, slow, fast)
        return loss, main_nll.reshape(1, 1, seq), mtp_nll.reshape(1, 1, seq)

    rep = P()
    in_specs = (P(None, "dp", None), P("pp", "dp", None), P("pp"), P("pp"), rep, rep, rep, rep, rep, rep, rep, rep)
    out_specs = (rep, P(None, "dp", None), P(None, "dp", None))
    return jax.shard_map(body, mesh=mesh, in_specs=in_specs, out_specs=out_specs, check_vma=False)
```

```python
import functools

import jax
import jax.numpy as jnp
from jax import lax
from jax.experimental import pallas as pl
from jax.experimental.pallas import tpu as pltpu
from jax.sharding import PartitionSpec as P

NORM_EPS = 1e-6
MTP_WEIGHT = 0.3
HEAD_ROWS = 128
LANES = 128
SUB = 8
K_TILE = 256
CAP = 24
PIECE = 512
MLP_BLOCK = 1024
E_GATE = 5
VMEM_LIMIT = 66_900_000
F32 = jnp.float32
BF16 = jnp.bfloat16
MESH = pl.DeviceIdType.MESH


def norm_f32(x_f):
    return x_f * lax.rsqrt(jnp.mean(x_f * x_f, axis=-1, keepdims=True) + NORM_EPS)


def iota(shape, dim):
    return lax.broadcasted_iota(jnp.int32, shape, dim)


def dot32(a, b):
    return jnp.dot(a, b, preferred_element_type=F32)


def mega_kernel(
    n_dp, n_pp, seq, cap,
    ids_ref, gf_ref, gh_ref, ge_ref, gm_ref, emb, w1h, w2h, wph, u1h, u2h, woh,
    out_ref, flag_out,
    w1, w2, u1, u2, wp, wo,
    ids_all, send_rows, recv_rows, xbuf, ybuf, xnb, hid, ebuf, hbuf, eall, zbuf, epart, xh, lg, mx, sm, pk,
    part_send, part_recv, ls_send, ls_recv, over_buf,
    wsem, ids_ss, ids_rs, row_ss, row_rs, x_ss, x_rs, e_ss, e_rs, h_ss, h_rs, f_ss, part_ss, part_rs, ls_ss, ls_rs,
    over_ss, over_rs, link_free,
):
    d = lax.axis_index("dp")
    p = lax.axis_index("pp")
    width = xbuf.shape[1]
    ffn = w1.shape[1]
    n_rows = emb.shape[1]
    half = seq // 2
    n_shard = n_pp // 2
    shard = lax.rem(p, n_shard)
    group = p // n_shard
    n_tiles = woh.shape[1] // LANES
    base_tiles = n_tiles // n_shard
    cols = w1.shape[1] + wo.shape[1]
    own_cols = wo.shape[1]
    n_piece = width // PIECE
    is_first = p == 0
    is_last = p == n_pp - 1
    k_main = n_rows // K_TILE * K_TILE
    k_pad = k_main + K_TILE
    n_id = seq + 2
    n_slots = n_dp * cap

    col0 = pl.multiple_of(shard * (base_tiles * LANES), LANES)
    tab_cp = pltpu.make_async_copy(emb.at[0], u2.at[pl.ds(0, n_rows), :], wsem.at[0])
    w1_cp = pltpu.make_async_copy(w1h.at[0, 0], w1, wsem.at[1])
    w2_cp = pltpu.make_async_copy(w2h.at[0, 0], w2, wsem.at[2])
    u1_cp = pltpu.make_async_copy(u1h, u1, wsem.at[3])
    u2_cp = pltpu.make_async_copy(u2h, u2, wsem.at[4])
    wp_cp = pltpu.make_async_copy(wph, wp, wsem.at[5])
    wo_cp = pltpu.make_async_copy(woh.at[:, pl.ds(col0 + ffn, own_cols)], wo, wsem.at[6])
    late_cp = pltpu.make_async_copy(woh.at[:, pl.ds(col0, ffn)], w1, wsem.at[7])

    @pl.when(is_first)
    def _():
        tab_cp.start()

    @pl.when(jnp.logical_not(is_first))
    def _():
        w1_cp.start()
        w2_cp.start()

    barrier = pltpu.get_barrier_semaphore()
    for k in range(1, n_dp):
        pl.semaphore_signal(barrier, inc=1, device_id={"dp": lax.rem(d + k, n_dp)}, device_id_type=MESH)
    for k in range(1, n_pp):
        pl.semaphore_signal(barrier, inc=1, device_id={"pp": lax.rem(p + k, n_pp)}, device_id_type=MESH)
    pl.semaphore_wait(barrier, n_dp - 1 + n_pp - 1)

    def ids_copy(owner, peer):
        return pltpu.make_async_remote_copy(
            src_ref=ids_ref.at[0], dst_ref=ids_all.at[owner], send_sem=ids_ss.at[peer], recv_sem=ids_rs.at[owner],
            device_id={"dp": peer}, device_id_type=MESH)

    @pl.when(is_first)
    def _():
        for k in range(1, n_dp):
            ids_copy(d, lax.rem(d + k, n_dp)).start()
        ids_all[d] = ids_ref[0]

    @pl.when(jnp.logical_not(is_first))
    def _():
        u1_cp.start()
        u2_cp.start()
        wp_cp.start()
        wo_cp.start()

    def row_copy(owner, peer):
        return pltpu.make_async_remote_copy(
            src_ref=send_rows.at[peer], dst_ref=recv_rows.at[owner], send_sem=row_ss.at[peer], recv_sem=row_rs.at[owner],
            device_id={"dp": peer}, device_id_type=MESH)

    def positions(row0, n):
        row = ids_ref[0]
        rr = iota((n, n_id), 0) + row0
        ll = iota((n, n_id), 1)
        pos = jnp.where(rr < seq, rr, rr - seq + 1)
        id_col = jnp.sum(jnp.where(ll == pos, jnp.broadcast_to(row, (n, n_id)), 0).astype(F32), axis=1, keepdims=True)
        src_col = jnp.zeros((n, 1), F32)
        src_row = jnp.zeros((1, n_id), F32)
        for k in range(1, n_dp):
            src_col = src_col + jnp.where(id_col >= float(k * n_rows), 1.0, 0.0)
            src_row = src_row + jnp.where(row >= k * n_rows, 1.0, 0.0)
        earlier = (jnp.broadcast_to(src_row, (n, n_id)) == src_col) & (ll < pos)
        rank_col = jnp.sum(jnp.where(earlier, 1.0, 0.0), axis=1, keepdims=True)
        where_col = jnp.where(rank_col < float(cap), src_col * float(cap) + rank_col, -1.0).astype(jnp.int32)
        return jnp.where(iota((n, n_slots), 1) == where_col, 1.0, 0.0).astype(BF16)

    @pl.when(is_first)
    def _():
        xnb[:, 0:n_slots] = positions(0, seq)
        eall[:, 0:n_slots] = positions(seq, seq)
        for k in range(1, n_dp):
            peer = lax.rem(d + k, n_dp)
            ids_copy(peer, peer).wait_recv()
        w1_cp.start()
        w2_cp.start()
        low = d * n_rows
        ids2 = ids_all[...].reshape(n_dp, n_id)
        lane2 = iota((n_dp, n_id), 1)
        valid = (ids2 >= low) & (ids2 < low + n_rows) & (lane2 < seq + 1)
        before = jnp.where(iota((n_id, n_id), 0) < iota((n_id, n_id), 1), 1.0, 0.0).astype(BF16)
        rank = dot32(jnp.where(valid, 1.0, 0.0).astype(BF16), before)
        key = jnp.where(valid, rank, -1.0)
        loc = jnp.where(valid, ids2 - low, 0).astype(F32)
        slot = iota((cap, n_id), 0).astype(F32)
        for b in range(0, n_dp, 2):
            picks = []
            for s in (b, b + 1):
                sel = key[s:s + 1, :] == slot
                idx = jnp.sum(jnp.where(sel, loc[s:s + 1, :] + 1.0, 0.0), axis=1, keepdims=True) - 1.0
                picks.append(idx)
            idx2 = jnp.concatenate(picks, axis=0).astype(jnp.int32)
            hot = jnp.where(iota((2 * cap, k_pad), 1) == idx2, 1.0, 0.0).astype(BF16)
            u1[b * cap:(b + 2) * cap, 0:k_pad] = hot
        tab_cp.wait()
        blk = min(512, width)
        for c in range(0, width, blk):
            tail = u2[k_main:k_pad, c:c + blk]
            tail = jnp.where(iota((K_TILE, blk), 0) < n_rows - k_main, tail.astype(F32), 0.0).astype(BF16)
            got = dot32(u1[0:n_slots, 0:k_main], u2[0:k_main, c:c + blk]) + dot32(u1[0:n_slots, k_main:k_pad], tail)
            for s in range(n_dp):
                send_rows[s, :, c:c + blk] = got[s * cap:(s + 1) * cap, :].astype(BF16)
        for k in range(1, n_dp):
            row_copy(d, lax.rem(d + k, n_dp)).start()
        recv_rows[d] = send_rows[d]
        u1_cp.start()
        u2_cp.start()
        wp_cp.start()
        wo_cp.start()
        for k in range(1, n_dp):
            peer = lax.rem(d + k, n_dp)
            row_copy(peer, peer).wait_recv()
        xbuf[...] = dot32(xnb[:, 0:n_slots], recv_rows[...].reshape(n_slots, width)).astype(BF16)

    def x_copy(i):
        part = pl.ds(i * PIECE, PIECE)
        return pltpu.make_async_remote_copy(
            src_ref=ybuf.at[:, part], dst_ref=xbuf.at[:, part], send_sem=x_ss.at[i], recv_sem=x_rs.at[i],
            device_id={"pp": lax.rem(p + 1, n_pp)}, device_id_type=MESH)

    h_peers = ((1, 0), (3, 0), (5, half), (6, half))

    def h_copy(j, i):
        to, row0 = h_peers[j]
        part = pl.ds(i * PIECE, PIECE)
        return pltpu.make_async_remote_copy(
            src_ref=ybuf.at[pl.ds(row0, half), part], dst_ref=hbuf.at[:, part], send_sem=h_ss.at[j, i], recv_sem=h_rs.at[i],
            device_id={"pp": to}, device_id_type=MESH)

    def f_copy(i):
        part = pl.ds(i * PIECE, PIECE)
        return pltpu.make_async_remote_copy(
            src_ref=hbuf.at[:, part], dst_ref=hbuf.at[:, part], send_sem=f_ss.at[i], recv_sem=h_rs.at[i],
            device_id={"pp": lax.rem(p + n_pp - 1, n_pp)}, device_id_type=MESH)

    def gelu_up(m, xn, w_up):
        for c in range(0, ffn, MLP_BLOCK):
            hid[0:m, c:c + MLP_BLOCK] = jax.nn.gelu(dot32(xn, w_up[:, c:c + MLP_BLOCK])).astype(BF16)

    w1_cp.wait()
    w2_cp.wait()

    @pl.when(jnp.logical_not(is_first))
    def _():
        for i in range(n_piece):
            x_copy(i).wait_recv()

    @pl.when(p == E_GATE)
    def _():
        pl.semaphore_signal(link_free, inc=1, device_id={"pp": 0}, device_id_type=MESH)

    xnb[...] = norm_f32(xbuf[...].astype(F32)).astype(BF16)
    gelu_up(seq, xnb[...], w1)
    for i in range(n_piece):
        c = i * PIECE
        out = xbuf[:, c:c + PIECE].astype(F32) + dot32(hid[...], w2[:, c:c + PIECE])
        ybuf[:, c:c + PIECE] = out.astype(BF16)

        @pl.when(jnp.logical_not(is_last))
        def _():
            x_copy(i).start()

        @pl.when(is_last)
        def _():
            for j in range(len(h_peers)):
                h_copy(j, i).start()

    late_cp.start()

    def e_copy(to):
        row0 = half * (to // n_shard)
        return pltpu.make_async_remote_copy(
            src_ref=eall.at[pl.ds(row0, half), :], dst_ref=ebuf, send_sem=e_ss.at[to], recv_sem=e_rs,
            device_id={"pp": to}, device_id_type=MESH)

    def over_copy(to):
        return pltpu.make_async_remote_copy(
            src_ref=over_buf.at[0], dst_ref=over_buf.at[1], send_sem=over_ss.at[to], recv_sem=over_rs,
            device_id={"pp": to}, device_id_type=MESH)

    @pl.when(is_first)
    def _():
        eall[...] = dot32(eall[:, 0:n_slots], recv_rows[...].reshape(n_slots, width)).astype(BF16)
        ids2 = ids_all[...].reshape(n_dp, n_id)
        used = iota((n_dp, n_id), 1) < seq + 1
        most = jnp.zeros((n_dp, 1), F32)
        for k in range(n_dp):
            hit = (ids2 >= k * n_rows) & (ids2 < (k + 1) * n_rows) & used
            most = jnp.maximum(most, jnp.sum(jnp.where(hit, 1.0, 0.0), axis=1, keepdims=True))
        over = jnp.broadcast_to(jnp.where(jnp.max(most, axis=0, keepdims=True) > cap, 1.0, 0.0), (SUB, LANES))
        over_buf[0] = over
        over_buf[1] = over
        ebuf[...] = eall[0:half, :]
        pl.semaphore_wait(link_free, 1)
        for to in range(1, n_pp):
            e_copy(to).start()
            over_copy(to).start()

    @pl.when(jnp.logical_not(is_first))
    def _():
        e_copy(1).wait_recv()
        over_copy(1).wait_recv()

    g_f, g_h, g_e, g_m = (ref[...].astype(F32).reshape(1, width) for ref in (gf_ref, gh_ref, ge_ref, gm_ref))

    wp_cp.wait()
    e_n = (norm_f32(ebuf[...].astype(F32)) * g_e).astype(BF16)
    epart[...] = dot32(e_n, wp[width:2 * width, :])
    u1_cp.wait()
    u2_cp.wait()
    wo_cp.wait()

    row_f = jnp.broadcast_to(ids_ref[0], (2 * half, n_id))
    rr = iota((2 * half, n_id), 0)
    at = jnp.where(rr < half, rr + 1, rr - half + 2) + group * half
    tgt = jnp.sum(jnp.where(iota((2 * half, n_id), 1) == at, row_f, 0).astype(F32), axis=1, keepdims=True)
    tgt = tgt.astype(jnp.int32) - shard * (base_tiles * LANES)
    tgt = jnp.broadcast_to(tgt, (2 * half, LANES))

    @pl.when(is_last)
    def _():
        hbuf[...] = ybuf[half:seq, :]

    @pl.when(jnp.logical_not(is_last))
    def _():
        for i in range(n_piece):
            h_copy(0, i).wait_recv()

            @pl.when((p == 1) | (p == 3) | (p == 5))
            def _():
                f_copy(i).start()

    h_f = norm_f32(hbuf[...].astype(F32))
    z_val = (dot32((h_f * g_h).astype(BF16), wp[0:width, :]) + epart[...]).astype(BF16)
    zbuf[...] = z_val
    xh[0:half, :] = (h_f * g_f).astype(BF16)
    xnb[0:half, :] = (norm_f32(z_val.astype(F32)) * g_m).astype(BF16)
    gelu_up(half, xnb[0:half, :], u1)
    z_out = (zbuf[...].astype(F32) + dot32(hid[0:half, :], u2[...])).astype(BF16)
    xh[half:2 * half, :] = (norm_f32(z_out.astype(F32)) * g_f).astype(BF16)

    lane = iota((2 * half, LANES), 1)
    tail_ok = jnp.broadcast_to(shard == n_shard - 1, (2 * half, LANES))
    blocks = [(wo, c, ffn + c, min(MLP_BLOCK, own_cols - c)) for c in range(0, own_cols, MLP_BLOCK)]
    blocks += [(w1, c, c, MLP_BLOCK) for c in range(0, ffn, MLP_BLOCK)]

    def logits_of(i):
        ref, c, _, n = blocks[i]
        lg[i % 2, :, 0:n] = dot32(xh[...], ref[:, c:c + n])

    def fold(i):
        _, _, start, n = blocks[i]
        tiles = []
        for t in range(0, n, LANES):
            val = lg[i % 2, :, t:t + LANES]
            tiles.append((start + t, val, start + t == cols - LANES))
        top = None if i == 0 else mx[...]
        for _, val, last in tiles:
            val = jnp.where(tail_ok, val, -jnp.inf) if last else val
            top = val if top is None else jnp.maximum(top, val)
        total = jnp.zeros_like(top) if i == 0 else sm[...] * jnp.exp(mx[...] - top)
        hit = jnp.zeros_like(top) if i == 0 else pk[...]
        for at_col, val, last in tiles:
            e_val = jnp.exp(val - top)
            match = lane == tgt - at_col
            if last:
                e_val = jnp.where(tail_ok, e_val, 0.0)
                match = match & tail_ok
            total = total + e_val
            hit = hit + jnp.where(match, val, 0.0)
        mx[...] = top
        sm[...] = total
        pk[...] = hit

    for i in range(len(blocks)):
        if i == len(blocks) - ffn // MLP_BLOCK:
            late_cp.wait()
        logits_of(i)
        if i:
            fold(i - 1)
    fold(len(blocks) - 1)

    eye = iota((2 * half, LANES), 0) == iota((2 * half, LANES), 1)

    def as_row(col):
        return jnp.sum(jnp.where(eye, jnp.broadcast_to(col, (2 * half, LANES)), 0.0), axis=0, keepdims=True)

    top = mx[...]
    m_col = jnp.max(top, axis=1, keepdims=True)
    s_col = jnp.sum(sm[...] * jnp.exp(top - m_col), axis=1, keepdims=True)
    p_col = jnp.sum(pk[...], axis=1, keepdims=True)
    sub = iota((SUB, LANES), 0)
    tile = jnp.where(sub == 0, as_row(m_col), jnp.where(sub == 1, as_row(s_col), as_row(p_col)))
    part_send[...] = tile
    part_recv[p] = tile

    def part_copy(owner, peer):
        return pltpu.make_async_remote_copy(
            src_ref=part_send, dst_ref=part_recv.at[owner], send_sem=part_ss.at[peer], recv_sem=part_rs.at[owner],
            device_id={"pp": peer}, device_id_type=MESH)

    for k in range(1, n_pp):
        part_copy(p, lax.rem(p + k, n_pp)).start()
    for k in range(1, n_pp):
        peer = lax.rem(p + k, n_pp)
        part_copy(peer, peer).wait_recv()

    def group_nll(g):
        got = [part_recv[g * n_shard + i] for i in range(n_shard)]
        best = functools.reduce(jnp.maximum, [t[0:1, :] for t in got])
        total = sum(t[1:2, :] * jnp.exp(t[0:1, :] - best) for t in got)
        return best + jnp.log(total) - sum(t[2:3, :] for t in got)

    nll_a = jnp.broadcast_to(group_nll(0), (SUB, LANES))
    nll_b = jnp.broadcast_to(group_nll(1), (SUB, LANES))
    low_lane = iota((SUB, LANES), 1) < half
    main = jnp.where(low_lane, nll_a, pltpu.roll(nll_b, half, 1))
    mtp = jnp.where(low_lane, pltpu.roll(nll_a, half, 1), nll_b)
    both = main + MTP_WEIGHT * mtp
    ls_send[...] = both
    ls_recv[d] = both

    def ls_copy(owner, peer):
        return pltpu.make_async_remote_copy(
            src_ref=ls_send, dst_ref=ls_recv.at[owner], send_sem=ls_ss.at[peer], recv_sem=ls_rs.at[owner],
            device_id={"dp": peer}, device_id_type=MESH)

    for k in range(1, n_dp):
        ls_copy(d, lax.rem(d + k, n_dp)).start()
    for k in range(1, n_dp):
        peer = lax.rem(d + k, n_dp)
        ls_copy(peer, peer).wait_recv()
    acc = ls_recv[0]
    for k in range(1, n_dp):
        acc = acc + ls_recv[k]
    loss = jnp.sum(acc, axis=1, keepdims=True) * (1.0 / (n_dp * seq))
    out_ref[...] = jnp.where(sub == 0, main, jnp.where(sub == 1, mtp, jnp.broadcast_to(loss, (SUB, LANES))))
    flag_out[0, 0] = jnp.max(over_buf[1]).astype(jnp.int32)

    for k in range(1, n_dp):
        ls_copy(d, lax.rem(d + k, n_dp)).wait_send()
    for k in range(1, n_pp):
        part_copy(p, lax.rem(p + k, n_pp)).wait_send()

    @pl.when(is_first)
    def _():
        for k in range(1, n_dp):
            ids_copy(d, lax.rem(d + k, n_dp)).wait_send()
            row_copy(d, lax.rem(d + k, n_dp)).wait_send()
        for to in range(1, n_pp):
            e_copy(to).wait_send()
            over_copy(to).wait_send()

    @pl.when(jnp.logical_not(is_last))
    def _():
        for i in range(n_piece):
            x_copy(i).wait_send()

    @pl.when((p == 1) | (p == 3) | (p == 5))
    def _():
        for i in range(n_piece):
            f_copy(i).wait_send()

    @pl.when(is_last)
    def _():
        for j in range(len(h_peers)):
            for i in range(n_piece):
                h_copy(j, i).wait_send()


def mega(n_dp, n_pp, seq, ids, gains, emb, w1, w2, wp, u1, u2, wo):
    width, ffn = w1.shape[2], w1.shape[3]
    n_tiles = wo.shape[1] // LANES
    n_shard = n_pp // 2
    cols = (n_tiles - (n_shard - 1) * (n_tiles // n_shard)) * LANES
    half = seq // 2
    n_piece = width // PIECE
    dma = pltpu.SemaphoreType.DMA
    tile = pltpu.VMEM((SUB, LANES), F32)
    vmem = pl.BlockSpec(memory_space=pltpu.VMEM)
    anys = pl.BlockSpec(memory_space=pl.ANY)
    act = pltpu.VMEM((seq, width), BF16)
    act_half = pltpu.VMEM((half, width), BF16)
    return pl.pallas_call(
        functools.partial(mega_kernel, n_dp, n_pp, seq, CAP),
        out_shape=(
            jax.ShapeDtypeStruct((SUB, LANES), F32),
            jax.ShapeDtypeStruct((1, 1), jnp.int32),
        ),
        in_specs=[vmem] * 5 + [anys] * 7,
        out_specs=(vmem, pl.BlockSpec(memory_space=pltpu.SMEM)),
        scratch_shapes=[
            pltpu.VMEM((width, ffn), BF16),
            pltpu.VMEM((ffn, width), BF16),
            pltpu.VMEM((width, ffn), BF16),
            pltpu.VMEM((ffn, width), BF16),
            pltpu.VMEM((2 * width, width), BF16),
            pltpu.VMEM((width, cols - ffn), BF16),
            pltpu.VMEM((n_dp, 1, seq + 2), jnp.int32),
            pltpu.VMEM((n_dp, CAP, width), BF16),
            pltpu.VMEM((n_dp, CAP, width), BF16),
            act, act, act,
            pltpu.VMEM((seq, ffn), BF16),
            act_half, act_half,
            act,
            act_half,
            pltpu.VMEM((half, width), F32),
            act,
            pltpu.VMEM((2, 2 * half, MLP_BLOCK), F32),
            pltpu.VMEM((2 * half, LANES), F32), pltpu.VMEM((2 * half, LANES), F32), pltpu.VMEM((2 * half, LANES), F32),
            tile, pltpu.VMEM((n_pp, SUB, LANES), F32),
            tile, pltpu.VMEM((n_dp, SUB, LANES), F32),
            pltpu.VMEM((2, SUB, LANES), F32),
            dma((8,)), dma((n_dp,)), dma((n_dp,)), dma((n_dp,)), dma((n_dp,)),
            dma((n_piece,)), dma((n_piece,)), dma((n_pp,)), dma(()), dma((4, n_piece)), dma((n_piece,)), dma((n_piece,)),
            dma((n_pp,)), dma((n_pp,)), dma((n_dp,)), dma((n_dp,)), dma((n_pp,)), dma(()), pltpu.SemaphoreType.REGULAR,
        ],
        compiler_params=pltpu.CompilerParams(collective_id=0, has_side_effects=True, vmem_limit_bytes=VMEM_LIMIT),
        name="mtp_eval",
    )(ids, *gains, emb, w1, w2, wp, u1, u2, wo)


def norm_plain(x_val):
    return norm_f32(x_val.astype(F32)).astype(BF16)


def norm_gain(x_val, gain_vec):
    return (norm_f32(x_val.astype(F32)) * gain_vec.astype(F32)).astype(BF16)


def mlp_add(x_val, normed, w_up, w_down):
    hidden = jax.nn.gelu(dot32(normed, w_up)).astype(BF16)
    return (x_val.astype(F32) + dot32(hidden, w_down)).astype(BF16)


def token_nll(normed, targets, w_out):
    n_rows, row_width = normed.shape
    n_blocks = n_rows // HEAD_ROWS

    def one_block(pair):
        block_rows, block_tgt = pair
        logits = dot32(block_rows, w_out)
        picked = jnp.take_along_axis(logits, block_tgt[:, None], axis=1)[:, 0]
        return jax.nn.logsumexp(logits, axis=1) - picked

    per_block = lax.map(one_block, (normed.reshape(n_blocks, HEAD_ROWS, row_width), targets.reshape(n_blocks, HEAD_ROWS)))
    return per_block.reshape(n_rows)


def any_ids(n_dp, n_pp, seq, ids, emb, w_one, w_two, gain_f, gain_h, gain_e, gain_m, w_proj, u_one, u_two, w_out):
    stage = lax.axis_index("pp")
    me = lax.axis_index("dp")
    n_rows, width = emb.shape
    ring = [(i, (i + 1) % n_dp) for i in range(n_dp)]
    want = ids[:seq + 1]

    def take(k, held, rows):
        local = want - lax.rem(me - k + n_dp, n_dp) * n_rows
        here = (local >= 0) & (local < n_rows)
        return jnp.where(here[:, None], held[jnp.clip(local, 0, n_rows - 1)], rows)

    def gather_step(k, carry):
        held, rows = carry
        rows = take(k, held, rows)
        return lax.ppermute(held, "dp", ring), rows

    rows = take(0, emb, jnp.zeros((seq + 1, width), BF16))
    _, rows = lax.fori_loop(1, n_dp, gather_step, (lax.ppermute(emb, "dp", ring), rows))
    to_next = [(i, i + 1) for i in range(n_pp - 1)]

    def tick(k, carry):
        x_val, _ = carry
        x_val = jnp.where((stage == 0) & (k == 0), rows[:seq], x_val)
        y_val = mlp_add(x_val, norm_plain(x_val), w_one, w_two)
        return lax.ppermute(y_val, "pp", to_next), y_val

    zero = jnp.zeros((seq, width), BF16)
    _, h_last = lax.fori_loop(0, n_pp, tick, (zero, zero))
    e_rows = lax.ppermute(rows[1:seq + 1], "pp", [(0, n_pp - 1)])
    main_nll = token_nll(norm_gain(h_last, gain_f), ids[1:seq + 1], w_out)
    z_sum = dot32(norm_gain(h_last, gain_h), w_proj[:width]) + dot32(norm_gain(e_rows, gain_e), w_proj[width:])
    z_val = z_sum.astype(BF16)
    z_val = mlp_add(z_val, norm_gain(z_val, gain_m), u_one, u_two)
    mtp_nll = token_nll(norm_gain(z_val, gain_f), ids[2:], w_out)
    is_last = stage == n_pp - 1
    main_nll = lax.psum(jnp.where(is_last, main_nll, 0.0), "pp")
    mtp_nll = lax.psum(jnp.where(is_last, mtp_nll, 0.0), "pp")
    total = lax.psum(jnp.sum(main_nll) + MTP_WEIGHT * jnp.sum(mtp_nll), "dp") / (n_dp * seq)
    return total, main_nll.reshape(1, seq), mtp_nll.reshape(1, seq)


def solution(mesh):
    n_pp = mesh.shape["pp"]
    n_dp = mesh.shape["dp"]

    def body(tok_ids, emb_s, w_one, w_two, gain_f, gain_h, gain_e, gain_m, w_proj, u_one, u_two, w_out):
        seq = tok_ids.shape[2] - 2
        gains = (gain_f, gain_h, gain_e, gain_m)
        packed, over = mega(n_dp, n_pp, seq, tok_ids, gains, emb_s, w_one, w_two, w_proj, u_one, u_two, w_out)

        def slow():
            total, main_nll, mtp_nll = any_ids(
                n_dp, n_pp, seq, tok_ids[0, 0], emb_s[0], w_one[0, 0], w_two[0, 0], *gains, w_proj, u_one, u_two, w_out)
            return jnp.concatenate([main_nll, mtp_nll, jnp.broadcast_to(total, (SUB - 2, seq))], axis=0)

        packed = lax.cond(over[0, 0] > 0, slow, lambda: packed)
        return packed[2, 0], packed[0:1].reshape(1, 1, seq), packed[1:2].reshape(1, 1, seq)

    rep = P()
    in_specs = (P(None, "dp", None), P("pp", "dp", None), P("pp"), P("pp"), rep, rep, rep, rep, rep, rep, rep, rep)
    out_specs = (rep, P(None, "dp", None), P(None, "dp", None))
    return jax.shard_map(body, mesh=mesh, in_specs=in_specs, out_specs=out_specs, check_vma=False)
```

```python
import functools

import jax
import jax.numpy as jnp
from jax import lax
from jax.experimental import pallas as pl
from jax.experimental.pallas import tpu as pltpu
from jax.sharding import PartitionSpec as P

NORM_EPS = 1e-6
MTP_WEIGHT = 0.3
HEAD_ROWS = 128
LANES = 128
SUB = 8
K_TILE = 256
CAP = 24
PIECE = 512
MLP_BLOCK = 1024
E_GATE = 5
VMEM_LIMIT = 66_900_000
F32 = jnp.float32
BF16 = jnp.bfloat16
MESH = pl.DeviceIdType.MESH


def norm_f32(x_f):
    return x_f * lax.rsqrt(jnp.mean(x_f * x_f, axis=-1, keepdims=True) + NORM_EPS)


def iota(shape, dim):
    return lax.broadcasted_iota(jnp.int32, shape, dim)


def dot32(a, b):
    return jnp.dot(a, b, preferred_element_type=F32)


def mega_kernel(
    n_dp, n_pp, seq, cap,
    ids_ref, gf_ref, gh_ref, ge_ref, gm_ref, emb, w1h, w2h, wph, u1h, u2h, woh,
    out_ref, flag_out,
    w1, w2, wp, wo,
    ids_all, send_rows, recv_rows, xbuf, ybuf, xnb, hid, ebuf, hbuf, eall, zbuf, epart, xh, lg, mx, sm, pk,
    part_send, part_recv, ls_send, ls_recv, over_buf,
    wsem, ids_ss, ids_rs, row_ss, row_rs, x_ss, x_rs, e_ss, e_rs, h_ss, h_rs, f_ss, part_ss, part_rs, ls_ss, ls_rs,
    over_ss, over_rs, link_free, push_ss, push_rs,
):
    d = lax.axis_index("dp")
    p = lax.axis_index("pp")
    width = xbuf.shape[1]
    ffn = w1.shape[2]
    n_rows = emb.shape[1]
    half = seq // 2
    n_shard = n_pp // 2
    shard = lax.rem(p, n_shard)
    group = p // n_shard
    n_tiles = woh.shape[1] // LANES
    base_tiles = n_tiles // n_shard
    cols = ffn + wo.shape[1]
    own_cols = wo.shape[1]
    n_piece = width // PIECE
    is_first = p == 0
    is_last = p == n_pp - 1
    even = lax.rem(p, 2) == 0
    lender = even & (p > 1)
    double = jnp.logical_not(even) & (p > 1)
    k_main = n_rows // K_TILE * K_TILE
    k_pad = k_main + K_TILE
    n_id = seq + 2
    n_slots = n_dp * cap

    col0 = pl.multiple_of(shard * (base_tiles * LANES), LANES)
    tab_cp = pltpu.make_async_copy(emb.at[0], w2.at[0, pl.ds(0, n_rows), :], wsem.at[0])
    w1_cp = pltpu.make_async_copy(w1h.at[0, 0], w1.at[1], wsem.at[1])
    w2_cp = pltpu.make_async_copy(w2h.at[0, 0], w2.at[1], wsem.at[2])
    u1_cp = pltpu.make_async_copy(u1h, w1.at[0], wsem.at[3])
    u2_cp = pltpu.make_async_copy(u2h, w2.at[0], wsem.at[4])
    wp_cp = pltpu.make_async_copy(wph, wp, wsem.at[5])
    wo_cp = pltpu.make_async_copy(woh.at[:, pl.ds(col0 + ffn, own_cols)], wo, wsem.at[6])
    late_cp = pltpu.make_async_copy(woh.at[:, pl.ds(col0, ffn)], w1.at[1], wsem.at[7])

    def push_copy(i):
        src, dst = ((w1h, w1), (w2h, w2))[i]
        return pltpu.make_async_remote_copy(
            src_ref=src.at[0, 0], dst_ref=dst.at[0], send_sem=push_ss.at[i], recv_sem=push_rs.at[i],
            device_id={"pp": lax.rem(p + 1, n_pp)}, device_id_type=MESH)

    @pl.when(is_first)
    def _():
        tab_cp.start()

    @pl.when(jnp.logical_not(even))
    def _():
        w1_cp.start()
        w2_cp.start()

    barrier = pltpu.get_barrier_semaphore()
    for k in range(1, n_dp):
        pl.semaphore_signal(barrier, inc=1, device_id={"dp": lax.rem(d + k, n_dp)}, device_id_type=MESH)
    for k in range(1, n_pp):
        pl.semaphore_signal(barrier, inc=1, device_id={"pp": lax.rem(p + k, n_pp)}, device_id_type=MESH)
    pl.semaphore_wait(barrier, n_dp - 1 + n_pp - 1)

    def ids_copy(owner, peer):
        return pltpu.make_async_remote_copy(
            src_ref=ids_ref.at[0], dst_ref=ids_all.at[owner], send_sem=ids_ss.at[peer], recv_sem=ids_rs.at[owner],
            device_id={"dp": peer}, device_id_type=MESH)

    @pl.when(is_first)
    def _():
        for k in range(1, n_dp):
            ids_copy(d, lax.rem(d + k, n_dp)).start()
        ids_all[d] = ids_ref[0]

    @pl.when(lender)
    def _():
        push_copy(0).start()
        push_copy(1).start()
        u1_cp.start()
        u2_cp.start()
        late_cp.start()

    @pl.when(p == 1)
    def _():
        u1_cp.start()
        u2_cp.start()

    @pl.when(jnp.logical_not(is_first))
    def _():
        wp_cp.start()
        wo_cp.start()

    n_y = 4
    n_z = n_dp // n_y
    offs = [(z, y) for z in range(n_z) for y in range(n_y)]
    offs.sort(key=lambda o: -(min(o[0], n_z - o[0]) + min(o[1], n_y - o[1])))
    order = [lax.rem(d // n_y + z, n_z) * n_y + lax.rem(d + y, n_y) for z, y in offs]

    def row_copy(owner, j):
        return pltpu.make_async_remote_copy(
            src_ref=send_rows.at[j], dst_ref=recv_rows.at[owner], send_sem=row_ss.at[j], recv_sem=row_rs.at[owner],
            device_id={"dp": order[j]}, device_id_type=MESH)

    def positions(row0, n):
        row = ids_ref[0]
        rr = iota((n, n_id), 0) + row0
        ll = iota((n, n_id), 1)
        pos = jnp.where(rr < seq, rr, rr - seq + 1)
        id_col = jnp.sum(jnp.where(ll == pos, jnp.broadcast_to(row, (n, n_id)), 0).astype(F32), axis=1, keepdims=True)
        src_col = jnp.zeros((n, 1), F32)
        src_row = jnp.zeros((1, n_id), F32)
        for k in range(1, n_dp):
            src_col = src_col + jnp.where(id_col >= float(k * n_rows), 1.0, 0.0)
            src_row = src_row + jnp.where(row >= k * n_rows, 1.0, 0.0)
        earlier = (jnp.broadcast_to(src_row, (n, n_id)) == src_col) & (ll < pos)
        rank_col = jnp.sum(jnp.where(earlier, 1.0, 0.0), axis=1, keepdims=True)
        where_col = jnp.where(rank_col < float(cap), src_col * float(cap) + rank_col, -1.0).astype(jnp.int32)
        return jnp.where(iota((n, n_slots), 1) == where_col, 1.0, 0.0).astype(BF16)

    @pl.when(is_first)
    def _():
        xnb[:, 0:n_slots] = positions(0, seq)
        eall[:, 0:n_slots] = positions(seq, seq)
        for k in range(1, n_dp):
            peer = lax.rem(d + k, n_dp)
            ids_copy(peer, peer).wait_recv()
        w1_cp.start()
        w2_cp.start()
        low = d * n_rows
        ids2 = jnp.concatenate([ids_all[peer] for peer in order], axis=0)
        lane2 = iota((n_dp, n_id), 1)
        valid = (ids2 >= low) & (ids2 < low + n_rows) & (lane2 < seq + 1)
        before = jnp.where(iota((n_id, n_id), 0) < iota((n_id, n_id), 1), 1.0, 0.0).astype(BF16)
        rank = dot32(jnp.where(valid, 1.0, 0.0).astype(BF16), before)
        key = jnp.where(valid, rank, -1.0)
        loc = jnp.where(valid, ids2 - low, 0).astype(F32)
        slot = iota((cap, n_id), 0).astype(F32)
        for b in range(0, n_dp, 2):
            picks = []
            for s in (b, b + 1):
                sel = key[s:s + 1, :] == slot
                idx = jnp.sum(jnp.where(sel, loc[s:s + 1, :] + 1.0, 0.0), axis=1, keepdims=True) - 1.0
                picks.append(idx)
            idx2 = jnp.concatenate(picks, axis=0).astype(jnp.int32)
            hot = jnp.where(iota((2 * cap, k_pad), 1) == idx2, 1.0, 0.0).astype(BF16)
            w1[0, b * cap:(b + 2) * cap, 0:k_pad] = hot
        tab_cp.wait()
        blk = min(512, width)
        n_half = n_dp // 2
        for h in range(2):
            r0, r1 = h * n_half * cap, (h + 1) * n_half * cap
            for c in range(0, width, blk):
                tail = w2[0, k_main:k_pad, c:c + blk]
                tail = jnp.where(iota((K_TILE, blk), 0) < n_rows - k_main, tail.astype(F32), 0.0).astype(BF16)
                got = dot32(w1[0, r0:r1, 0:k_main], w2[0, 0:k_main, c:c + blk]) + dot32(w1[0, r0:r1, k_main:k_pad], tail)
                for s in range(n_half):
                    send_rows[h * n_half + s, :, c:c + blk] = got[s * cap:(s + 1) * cap, :].astype(BF16)
            for j in range(h * n_half, min((h + 1) * n_half, n_dp - 1)):
                row_copy(d, j).start()
        recv_rows[d] = send_rows[n_dp - 1]
        u1_cp.start()
        u2_cp.start()
        wp_cp.start()
        wo_cp.start()
        for j in range(n_dp - 1):
            row_copy(order[j], j).wait_recv()
        xbuf[...] = dot32(xnb[:, 0:n_slots], recv_rows[...].reshape(n_slots, width)).astype(BF16)

    def x_copy(i):
        part = pl.ds(i * PIECE, PIECE)
        return pltpu.make_async_remote_copy(
            src_ref=ybuf.at[:, part], dst_ref=xbuf.at[:, part], send_sem=x_ss.at[i], recv_sem=x_rs.at[i],
            device_id={"pp": jnp.where(is_first, 1, lax.rem(p + 2, n_pp))}, device_id_type=MESH)

    h_peers = ((3, 0), (1, 0), (5, half), (6, half))

    def h_copy(j, i):
        to, row0 = h_peers[j]
        part = pl.ds(i * PIECE, PIECE)
        return pltpu.make_async_remote_copy(
            src_ref=ybuf.at[pl.ds(row0, half), part], dst_ref=hbuf.at[:, part], send_sem=h_ss.at[j, i], recv_sem=h_rs.at[i],
            device_id={"pp": to}, device_id_type=MESH)

    def f_copy(i):
        part = pl.ds(i * PIECE, PIECE)
        return pltpu.make_async_remote_copy(
            src_ref=hbuf.at[:, part], dst_ref=hbuf.at[:, part], send_sem=f_ss.at[i], recv_sem=h_rs.at[i],
            device_id={"pp": lax.rem(p + n_pp - 1, n_pp)}, device_id_type=MESH)

    def gelu_up(m, xn, slot):
        for c in range(0, ffn, MLP_BLOCK):
            hid[0:m, c:c + MLP_BLOCK] = jax.nn.gelu(dot32(xn, w1[slot, :, c:c + MLP_BLOCK])).astype(BF16)

    def stage(turn, carry):
        lent = turn == 0

        @pl.when(jnp.where(lent, double, jnp.logical_not(lender)))
        def _():
            @pl.when(lent)
            def _():
                push_copy(0).wait_recv()
                push_copy(1).wait_recv()

            @pl.when(jnp.logical_not(lent))
            def _():
                w1_cp.wait()
                w2_cp.wait()

            @pl.when(lent | (p == 1))
            def _():
                for i in range(n_piece):
                    x_copy(i).wait_recv()

            @pl.when(lent & (p == E_GATE))
            def _():
                pl.semaphore_signal(link_free, inc=1, device_id={"pp": 0}, device_id_type=MESH)

            xnb[...] = norm_f32(xbuf[...].astype(F32)).astype(BF16)
            gelu_up(seq, xnb[...], turn)
            for i in range(n_piece):
                c = i * PIECE
                out = xbuf[:, c:c + PIECE].astype(F32) + dot32(hid[...], w2[turn, :, c:c + PIECE])
                ybuf[:, c:c + PIECE] = out.astype(BF16)

                @pl.when(jnp.logical_not(lent | is_last))
                def _():
                    x_copy(i).start()

                @pl.when(jnp.logical_not(lent) & is_last)
                def _():
                    for j in range(len(h_peers)):
                        h_copy(j, i).start()

            @pl.when(lent)
            def _():
                u1_cp.start()
                u2_cp.start()
                xbuf[...] = ybuf[...]

            @pl.when(jnp.logical_not(lent))
            def _():
                late_cp.start()

        return carry

    lax.fori_loop(0, 2, stage, 0)

    def e_copy(to):
        row0 = half * (to // n_shard)
        return pltpu.make_async_remote_copy(
            src_ref=eall.at[pl.ds(row0, half), :], dst_ref=ebuf, send_sem=e_ss.at[to], recv_sem=e_rs,
            device_id={"pp": to}, device_id_type=MESH)

    def over_copy(to):
        return pltpu.make_async_remote_copy(
            src_ref=over_buf.at[0], dst_ref=over_buf.at[1], send_sem=over_ss.at[to], recv_sem=over_rs,
            device_id={"pp": to}, device_id_type=MESH)

    @pl.when(is_first)
    def _():
        eall[...] = dot32(eall[:, 0:n_slots], recv_rows[...].reshape(n_slots, width)).astype(BF16)
        ids2 = ids_all[...].reshape(n_dp, n_id)
        used = iota((n_dp, n_id), 1) < seq + 1
        most = jnp.zeros((n_dp, 1), F32)
        for k in range(n_dp):
            hit = (ids2 >= k * n_rows) & (ids2 < (k + 1) * n_rows) & used
            most = jnp.maximum(most, jnp.sum(jnp.where(hit, 1.0, 0.0), axis=1, keepdims=True))
        over = jnp.broadcast_to(jnp.where(jnp.max(most, axis=0, keepdims=True) > cap, 1.0, 0.0), (SUB, LANES))
        over_buf[0] = over
        over_buf[1] = over
        ebuf[...] = eall[0:half, :]
        pl.semaphore_wait(link_free, 1)
        for to in range(1, n_pp):
            e_copy(to).start()
            over_copy(to).start()

    @pl.when(jnp.logical_not(is_first))
    def _():
        e_copy(1).wait_recv()
        over_copy(1).wait_recv()

    g_f, g_h, g_e, g_m = (ref[...].astype(F32).reshape(1, width) for ref in (gf_ref, gh_ref, ge_ref, gm_ref))

    wp_cp.wait()
    e_n = (norm_f32(ebuf[...].astype(F32)) * g_e).astype(BF16)
    epart[...] = dot32(e_n, wp[width:2 * width, :])
    u1_cp.wait()
    u2_cp.wait()
    wo_cp.wait()

    row_f = jnp.broadcast_to(ids_ref[0], (2 * half, n_id))
    rr = iota((2 * half, n_id), 0)
    at = jnp.where(rr < half, rr + 1, rr - half + 2) + group * half
    tgt = jnp.sum(jnp.where(iota((2 * half, n_id), 1) == at, row_f, 0).astype(F32), axis=1, keepdims=True)
    tgt = tgt.astype(jnp.int32) - shard * (base_tiles * LANES)
    tgt = jnp.broadcast_to(tgt, (2 * half, LANES))

    @pl.when(is_last)
    def _():
        hbuf[...] = ybuf[half:seq, :]

    @pl.when(jnp.logical_not(is_last))
    def _():
        for i in range(n_piece):
            h_copy(0, i).wait_recv()

            @pl.when((p == 1) | (p == 3) | (p == 5))
            def _():
                f_copy(i).start()

    h_f = norm_f32(hbuf[...].astype(F32))
    z_val = (dot32((h_f * g_h).astype(BF16), wp[0:width, :]) + epart[...]).astype(BF16)
    zbuf[...] = z_val
    xh[0:half, :] = (h_f * g_f).astype(BF16)
    xnb[0:half, :] = (norm_f32(z_val.astype(F32)) * g_m).astype(BF16)
    gelu_up(half, xnb[0:half, :], 0)
    z_out = (zbuf[...].astype(F32) + dot32(hid[0:half, :], w2[0])).astype(BF16)
    xh[half:2 * half, :] = (norm_f32(z_out.astype(F32)) * g_f).astype(BF16)

    lane = iota((2 * half, LANES), 1)
    tail_ok = jnp.broadcast_to(shard == n_shard - 1, (2 * half, LANES))
    blocks = [(wo, c, ffn + c, min(MLP_BLOCK, own_cols - c)) for c in range(0, own_cols, MLP_BLOCK)]
    blocks += [(w1.at[1], c, c, MLP_BLOCK) for c in range(0, ffn, MLP_BLOCK)]

    def logits_of(i):
        ref, c, _, n = blocks[i]
        lg[i % 2, :, 0:n] = dot32(xh[...], ref[:, c:c + n])

    def fold(i):
        _, _, start, n = blocks[i]
        tiles = []
        for t in range(0, n, LANES):
            val = lg[i % 2, :, t:t + LANES]
            tiles.append((start + t, val, start + t == cols - LANES))
        top = None if i == 0 else mx[...]
        for _, val, last in tiles:
            val = jnp.where(tail_ok, val, -jnp.inf) if last else val
            top = val if top is None else jnp.maximum(top, val)
        total = jnp.zeros_like(top) if i == 0 else sm[...] * jnp.exp(mx[...] - top)
        hit = jnp.zeros_like(top) if i == 0 else pk[...]
        for at_col, val, last in tiles:
            e_val = jnp.exp(val - top)
            match = lane == tgt - at_col
            if last:
                e_val = jnp.where(tail_ok, e_val, 0.0)
                match = match & tail_ok
            total = total + e_val
            hit = hit + jnp.where(match, val, 0.0)
        mx[...] = top
        sm[...] = total
        pk[...] = hit

    for i in range(len(blocks)):
        if i == len(blocks) - ffn // MLP_BLOCK:
            late_cp.wait()
        logits_of(i)
        if i:
            fold(i - 1)
    fold(len(blocks) - 1)

    eye = iota((2 * half, LANES), 0) == iota((2 * half, LANES), 1)

    def as_row(col):
        return jnp.sum(jnp.where(eye, jnp.broadcast_to(col, (2 * half, LANES)), 0.0), axis=0, keepdims=True)

    top = mx[...]
    m_col = jnp.max(top, axis=1, keepdims=True)
    s_col = jnp.sum(sm[...] * jnp.exp(top - m_col), axis=1, keepdims=True)
    p_col = jnp.sum(pk[...], axis=1, keepdims=True)
    sub = iota((SUB, LANES), 0)
    tile = jnp.where(sub == 0, as_row(m_col), jnp.where(sub == 1, as_row(s_col), as_row(p_col)))
    part_send[...] = tile
    part_recv[p] = tile

    def part_copy(owner, peer):
        return pltpu.make_async_remote_copy(
            src_ref=part_send, dst_ref=part_recv.at[owner], send_sem=part_ss.at[peer], recv_sem=part_rs.at[owner],
            device_id={"pp": peer}, device_id_type=MESH)

    for k in range(1, n_pp):
        part_copy(p, lax.rem(p + k, n_pp)).start()
    for k in range(1, n_pp):
        peer = lax.rem(p + k, n_pp)
        part_copy(peer, peer).wait_recv()

    def group_nll(g):
        got = [part_recv[g * n_shard + i] for i in range(n_shard)]
        best = functools.reduce(jnp.maximum, [t[0:1, :] for t in got])
        total = sum(t[1:2, :] * jnp.exp(t[0:1, :] - best) for t in got)
        return best + jnp.log(total) - sum(t[2:3, :] for t in got)

    nll_a = jnp.broadcast_to(group_nll(0), (SUB, LANES))
    nll_b = jnp.broadcast_to(group_nll(1), (SUB, LANES))
    low_lane = iota((SUB, LANES), 1) < half
    main = jnp.where(low_lane, nll_a, pltpu.roll(nll_b, half, 1))
    mtp = jnp.where(low_lane, pltpu.roll(nll_a, half, 1), nll_b)
    both = main + MTP_WEIGHT * mtp
    ls_send[...] = both
    ls_recv[d] = both

    def ls_copy(owner, peer):
        return pltpu.make_async_remote_copy(
            src_ref=ls_send, dst_ref=ls_recv.at[owner], send_sem=ls_ss.at[peer], recv_sem=ls_rs.at[owner],
            device_id={"dp": peer}, device_id_type=MESH)

    for k in range(1, n_dp):
        ls_copy(d, lax.rem(d + k, n_dp)).start()
    for k in range(1, n_dp):
        peer = lax.rem(d + k, n_dp)
        ls_copy(peer, peer).wait_recv()
    acc = ls_recv[0]
    for k in range(1, n_dp):
        acc = acc + ls_recv[k]
    loss = jnp.sum(acc, axis=1, keepdims=True) * (1.0 / (n_dp * seq))
    out_ref[...] = jnp.where(sub == 0, main, jnp.where(sub == 1, mtp, jnp.broadcast_to(loss, (SUB, LANES))))
    flag_out[0, 0] = jnp.max(over_buf[1]).astype(jnp.int32)

    for k in range(1, n_dp):
        ls_copy(d, lax.rem(d + k, n_dp)).wait_send()
    for k in range(1, n_pp):
        part_copy(p, lax.rem(p + k, n_pp)).wait_send()

    @pl.when(is_first)
    def _():
        for k in range(1, n_dp):
            ids_copy(d, lax.rem(d + k, n_dp)).wait_send()
        for j in range(n_dp - 1):
            row_copy(d, j).wait_send()
        for to in range(1, n_pp):
            e_copy(to).wait_send()
            over_copy(to).wait_send()

    @pl.when(jnp.logical_not(is_last | lender))
    def _():
        for i in range(n_piece):
            x_copy(i).wait_send()

    @pl.when(lender)
    def _():
        push_copy(0).wait_send()
        push_copy(1).wait_send()

    @pl.when((p == 1) | (p == 3) | (p == 5))
    def _():
        for i in range(n_piece):
            f_copy(i).wait_send()

    @pl.when(is_last)
    def _():
        for j in range(len(h_peers)):
            for i in range(n_piece):
                h_copy(j, i).wait_send()


def mega(n_dp, n_pp, seq, ids, gains, emb, w1, w2, wp, u1, u2, wo):
    width, ffn = w1.shape[2], w1.shape[3]
    n_tiles = wo.shape[1] // LANES
    n_shard = n_pp // 2
    cols = (n_tiles - (n_shard - 1) * (n_tiles // n_shard)) * LANES
    half = seq // 2
    n_piece = width // PIECE
    dma = pltpu.SemaphoreType.DMA
    tile = pltpu.VMEM((SUB, LANES), F32)
    vmem = pl.BlockSpec(memory_space=pltpu.VMEM)
    anys = pl.BlockSpec(memory_space=pl.ANY)
    act = pltpu.VMEM((seq, width), BF16)
    act_half = pltpu.VMEM((half, width), BF16)
    return pl.pallas_call(
        functools.partial(mega_kernel, n_dp, n_pp, seq, CAP),
        out_shape=(
            jax.ShapeDtypeStruct((SUB, LANES), F32),
            jax.ShapeDtypeStruct((1, 1), jnp.int32),
        ),
        in_specs=[vmem] * 5 + [anys] * 7,
        out_specs=(vmem, pl.BlockSpec(memory_space=pltpu.SMEM)),
        scratch_shapes=[
            pltpu.VMEM((2, width, ffn), BF16),
            pltpu.VMEM((2, ffn, width), BF16),
            pltpu.VMEM((2 * width, width), BF16),
            pltpu.VMEM((width, cols - ffn), BF16),
            pltpu.VMEM((n_dp, 1, seq + 2), jnp.int32),
            pltpu.VMEM((n_dp, CAP, width), BF16),
            pltpu.VMEM((n_dp, CAP, width), BF16),
            act, act, act,
            pltpu.VMEM((seq, ffn), BF16),
            act_half, act_half,
            act,
            act_half,
            pltpu.VMEM((half, width), F32),
            act,
            pltpu.VMEM((2, 2 * half, MLP_BLOCK), F32),
            pltpu.VMEM((2 * half, LANES), F32), pltpu.VMEM((2 * half, LANES), F32), pltpu.VMEM((2 * half, LANES), F32),
            tile, pltpu.VMEM((n_pp, SUB, LANES), F32),
            tile, pltpu.VMEM((n_dp, SUB, LANES), F32),
            pltpu.VMEM((2, SUB, LANES), F32),
            dma((8,)), dma((n_dp,)), dma((n_dp,)), dma((n_dp,)), dma((n_dp,)),
            dma((n_piece,)), dma((n_piece,)), dma((n_pp,)), dma(()), dma((4, n_piece)), dma((n_piece,)), dma((n_piece,)),
            dma((n_pp,)), dma((n_pp,)), dma((n_dp,)), dma((n_dp,)), dma((n_pp,)), dma(()), pltpu.SemaphoreType.REGULAR,
            dma((2,)), dma((2,)),
        ],
        compiler_params=pltpu.CompilerParams(collective_id=0, has_side_effects=True, vmem_limit_bytes=VMEM_LIMIT),
        name="mtp_eval",
    )(ids, *gains, emb, w1, w2, wp, u1, u2, wo)


def norm_plain(x_val):
    return norm_f32(x_val.astype(F32)).astype(BF16)


def norm_gain(x_val, gain_vec):
    return (norm_f32(x_val.astype(F32)) * gain_vec.astype(F32)).astype(BF16)


def mlp_add(x_val, normed, w_up, w_down):
    hidden = jax.nn.gelu(dot32(normed, w_up)).astype(BF16)
    return (x_val.astype(F32) + dot32(hidden, w_down)).astype(BF16)


def token_nll(normed, targets, w_out):
    n_rows, row_width = normed.shape
    n_blocks = n_rows // HEAD_ROWS

    def one_block(pair):
        block_rows, block_tgt = pair
        logits = dot32(block_rows, w_out)
        picked = jnp.take_along_axis(logits, block_tgt[:, None], axis=1)[:, 0]
        return jax.nn.logsumexp(logits, axis=1) - picked

    per_block = lax.map(one_block, (normed.reshape(n_blocks, HEAD_ROWS, row_width), targets.reshape(n_blocks, HEAD_ROWS)))
    return per_block.reshape(n_rows)


def any_ids(n_dp, n_pp, seq, ids, emb, w_one, w_two, gain_f, gain_h, gain_e, gain_m, w_proj, u_one, u_two, w_out):
    stage = lax.axis_index("pp")
    me = lax.axis_index("dp")
    n_rows, width = emb.shape
    ring = [(i, (i + 1) % n_dp) for i in range(n_dp)]
    want = ids[:seq + 1]

    def take(k, held, rows):
        local = want - lax.rem(me - k + n_dp, n_dp) * n_rows
        here = (local >= 0) & (local < n_rows)
        return jnp.where(here[:, None], held[jnp.clip(local, 0, n_rows - 1)], rows)

    def gather_step(k, carry):
        held, rows = carry
        rows = take(k, held, rows)
        return lax.ppermute(held, "dp", ring), rows

    rows = take(0, emb, jnp.zeros((seq + 1, width), BF16))
    _, rows = lax.fori_loop(1, n_dp, gather_step, (lax.ppermute(emb, "dp", ring), rows))
    to_next = [(i, i + 1) for i in range(n_pp - 1)]

    def tick(k, carry):
        x_val, _ = carry
        x_val = jnp.where((stage == 0) & (k == 0), rows[:seq], x_val)
        y_val = mlp_add(x_val, norm_plain(x_val), w_one, w_two)
        return lax.ppermute(y_val, "pp", to_next), y_val

    zero = jnp.zeros((seq, width), BF16)
    _, h_last = lax.fori_loop(0, n_pp, tick, (zero, zero))
    e_rows = lax.ppermute(rows[1:seq + 1], "pp", [(0, n_pp - 1)])
    main_nll = token_nll(norm_gain(h_last, gain_f), ids[1:seq + 1], w_out)
    z_sum = dot32(norm_gain(h_last, gain_h), w_proj[:width]) + dot32(norm_gain(e_rows, gain_e), w_proj[width:])
    z_val = z_sum.astype(BF16)
    z_val = mlp_add(z_val, norm_gain(z_val, gain_m), u_one, u_two)
    mtp_nll = token_nll(norm_gain(z_val, gain_f), ids[2:], w_out)
    is_last = stage == n_pp - 1
    main_nll = lax.psum(jnp.where(is_last, main_nll, 0.0), "pp")
    mtp_nll = lax.psum(jnp.where(is_last, mtp_nll, 0.0), "pp")
    total = lax.psum(jnp.sum(main_nll) + MTP_WEIGHT * jnp.sum(mtp_nll), "dp") / (n_dp * seq)
    return total, main_nll.reshape(1, seq), mtp_nll.reshape(1, seq)


def solution(mesh):
    n_pp = mesh.shape["pp"]
    n_dp = mesh.shape["dp"]

    def body(tok_ids, emb_s, w_one, w_two, gain_f, gain_h, gain_e, gain_m, w_proj, u_one, u_two, w_out):
        seq = tok_ids.shape[2] - 2
        gains = (gain_f, gain_h, gain_e, gain_m)
        packed, over = mega(n_dp, n_pp, seq, tok_ids, gains, emb_s, w_one, w_two, w_proj, u_one, u_two, w_out)

        def slow():
            total, main_nll, mtp_nll = any_ids(
                n_dp, n_pp, seq, tok_ids[0, 0], emb_s[0], w_one[0, 0], w_two[0, 0], *gains, w_proj, u_one, u_two, w_out)
            return jnp.concatenate([main_nll, mtp_nll, jnp.broadcast_to(total, (SUB - 2, seq))], axis=0)

        packed = lax.cond(over[0, 0] > 0, slow, lambda: packed)
        return packed[2, 0], packed[0:1].reshape(1, 1, seq), packed[1:2].reshape(1, 1, seq)

    rep = P()
    in_specs = (P(None, "dp", None), P("pp", "dp", None), P("pp"), P("pp"), rep, rep, rep, rep, rep, rep, rep, rep)
    out_specs = (rep, P(None, "dp", None), P(None, "dp", None))
    return jax.shard_map(body, mesh=mesh, in_specs=in_specs, out_specs=out_specs, check_vma=False)
```

```python
import functools

import jax
import jax.numpy as jnp
from jax import lax
from jax.experimental import pallas as pl
from jax.experimental.pallas import tpu as pltpu
from jax.sharding import PartitionSpec as P

NORM_EPS = 1e-6
MTP_WEIGHT = 0.3
HEAD_ROWS = 128
LANES = 128
SUB = 8
K_TILE = 256
CAP = 24
PIECE = 512
MLP_BLOCK = 1024
E_GATE = 5
VMEM_LIMIT = 66_900_000
F32 = jnp.float32
BF16 = jnp.bfloat16
MESH = pl.DeviceIdType.MESH


def norm_f32(x_f):
    return x_f * lax.rsqrt(jnp.mean(x_f * x_f, axis=-1, keepdims=True) + NORM_EPS)


def iota(shape, dim):
    return lax.broadcasted_iota(jnp.int32, shape, dim)


def dot32(a, b):
    return jnp.dot(a, b, preferred_element_type=F32)


def mega_kernel(
    n_dp, n_pp, seq, cap,
    ids_ref, gf_ref, gh_ref, ge_ref, gm_ref, emb, w1h, w2h, wph, u1h, u2h, woh,
    out_ref, flag_out,
    w1, w2, wp, wo,
    ids_all, send_rows, recv_rows, xbuf, ybuf, xnb, hid, ebuf, hbuf, eall, zbuf, epart, xh, lg, mx, sm, pk,
    part_send, part_recv, ls_send, ls_recv, over_buf,
    wsem, ids_ss, ids_rs, row_ss, row_rs, x_ss, x_rs, e_ss, e_rs, h_ss, h_rs, f_ss, part_ss, part_rs, ls_ss, ls_rs,
    over_ss, over_rs, link_free, push_ss, push_rs,
):
    d = lax.axis_index("dp")
    p = lax.axis_index("pp")
    width = xbuf.shape[1]
    ffn = w1.shape[2]
    n_rows = emb.shape[1]
    half = seq // 2
    n_shard = n_pp // 2
    shard = lax.rem(p, n_shard)
    group = p // n_shard
    n_tiles = woh.shape[1] // LANES
    base_tiles = n_tiles // n_shard
    cols = ffn + wo.shape[1]
    own_cols = wo.shape[1]
    n_piece = width // PIECE
    is_first = p == 0
    is_last = p == n_pp - 1
    even = lax.rem(p, 2) == 0
    lender = even & (p > 1)
    double = jnp.logical_not(even) & (p > 1)
    k_main = n_rows // K_TILE * K_TILE
    k_pad = k_main + K_TILE
    n_id = seq + 2
    n_slots = n_dp * cap

    col0 = pl.multiple_of(shard * (base_tiles * LANES), LANES)
    tab_cp = pltpu.make_async_copy(emb.at[0], w2.at[0, pl.ds(0, n_rows), :], wsem.at[0])
    w1_cp = pltpu.make_async_copy(w1h.at[0, 0], w1.at[1], wsem.at[1])
    w2_cp = pltpu.make_async_copy(w2h.at[0, 0], w2.at[1], wsem.at[2])
    u1_cp = pltpu.make_async_copy(u1h, w1.at[0], wsem.at[3])
    u2_cp = pltpu.make_async_copy(u2h, w2.at[0], wsem.at[4])
    wp_cp = pltpu.make_async_copy(wph, wp, wsem.at[5])
    wo_cp = pltpu.make_async_copy(woh.at[:, pl.ds(col0 + ffn, own_cols)], wo, wsem.at[6])
    late_cp = pltpu.make_async_copy(woh.at[:, pl.ds(col0, ffn)], w1.at[1], wsem.at[7])

    def push_copy(i):
        src, dst = ((w1h, w1), (w2h, w2))[i]
        return pltpu.make_async_remote_copy(
            src_ref=src.at[0, 0], dst_ref=dst.at[0], send_sem=push_ss.at[i], recv_sem=push_rs.at[i],
            device_id={"pp": lax.rem(p + 1, n_pp)}, device_id_type=MESH)

    @pl.when(is_first)
    def _():
        tab_cp.start()

    @pl.when(jnp.logical_not(even))
    def _():
        w1_cp.start()
        w2_cp.start()

    barrier = pltpu.get_barrier_semaphore()
    for k in range(1, n_dp):
        pl.semaphore_signal(barrier, inc=1, device_id={"dp": lax.rem(d + k, n_dp)}, device_id_type=MESH)
    for k in range(1, n_pp):
        pl.semaphore_signal(barrier, inc=1, device_id={"pp": lax.rem(p + k, n_pp)}, device_id_type=MESH)
    @pl.when(even)
    def _():
        for k in range(1, n_dp):
            pl.semaphore_signal(
                barrier, inc=1, device_id={"dp": lax.rem(d + k, n_dp), "pp": lax.rem(p + 1, n_pp)}, device_id_type=MESH)

    pl.semaphore_wait(barrier, n_pp - 1 + jnp.where(even, 1, 2) * (n_dp - 1))

    def ids_copy(owner, peer):
        return pltpu.make_async_remote_copy(
            src_ref=ids_ref.at[0], dst_ref=ids_all.at[owner], send_sem=ids_ss.at[peer], recv_sem=ids_rs.at[owner],
            device_id={"dp": peer, "pp": 0}, device_id_type=MESH)

    @pl.when(p == 1)
    def _():
        for k in range(1, n_dp):
            ids_copy(d, lax.rem(d + k, n_dp)).start()

    @pl.when(is_first)
    def _():
        ids_all[d] = ids_ref[0]

    @pl.when(lender)
    def _():
        push_copy(0).start()
        push_copy(1).start()
        u1_cp.start()
        u2_cp.start()
        late_cp.start()

    @pl.when(p == 1)
    def _():
        u1_cp.start()
        u2_cp.start()

    @pl.when(jnp.logical_not(is_first))
    def _():
        wp_cp.start()
        wo_cp.start()

    n_y = 4
    n_z = n_dp // n_y
    offs = [(z, y) for z in range(n_z) for y in range(n_y)]
    offs.sort(key=lambda o: -(min(o[0], n_z - o[0]) + min(o[1], n_y - o[1])))
    order = [lax.rem(d // n_y + z, n_z) * n_y + lax.rem(d + y, n_y) for z, y in offs]

    def row_copy(owner, j):
        return pltpu.make_async_remote_copy(
            src_ref=send_rows.at[j], dst_ref=recv_rows.at[owner], send_sem=row_ss.at[j], recv_sem=row_rs.at[owner],
            device_id={"dp": order[j]}, device_id_type=MESH)

    def positions(row0, n):
        row = ids_ref[0]
        rr = iota((n, n_id), 0) + row0
        ll = iota((n, n_id), 1)
        pos = jnp.where(rr < seq, rr, rr - seq + 1)
        id_col = jnp.sum(jnp.where(ll == pos, jnp.broadcast_to(row, (n, n_id)), 0).astype(F32), axis=1, keepdims=True)
        src_col = jnp.zeros((n, 1), F32)
        src_row = jnp.zeros((1, n_id), F32)
        for k in range(1, n_dp):
            src_col = src_col + jnp.where(id_col >= float(k * n_rows), 1.0, 0.0)
            src_row = src_row + jnp.where(row >= k * n_rows, 1.0, 0.0)
        earlier = (jnp.broadcast_to(src_row, (n, n_id)) == src_col) & (ll < pos)
        rank_col = jnp.sum(jnp.where(earlier, 1.0, 0.0), axis=1, keepdims=True)
        where_col = jnp.where(rank_col < float(cap), src_col * float(cap) + rank_col, -1.0).astype(jnp.int32)
        return jnp.where(iota((n, n_slots), 1) == where_col, 1.0, 0.0).astype(BF16)

    @pl.when(is_first)
    def _():
        xnb[:, 0:n_slots] = positions(0, seq)
        eall[:, 0:n_slots] = positions(seq, seq)
        for k in range(1, n_dp):
            peer = lax.rem(d + k, n_dp)
            ids_copy(peer, peer).wait_recv()
        w1_cp.start()
        w2_cp.start()
        low = d * n_rows
        ids2 = jnp.concatenate([ids_all[peer] for peer in order], axis=0)
        lane2 = iota((n_dp, n_id), 1)
        valid = (ids2 >= low) & (ids2 < low + n_rows) & (lane2 < seq + 1)
        before = jnp.where(iota((n_id, n_id), 0) < iota((n_id, n_id), 1), 1.0, 0.0).astype(BF16)
        rank = dot32(jnp.where(valid, 1.0, 0.0).astype(BF16), before)
        key = jnp.where(valid, rank, -1.0)
        loc = jnp.where(valid, ids2 - low, 0).astype(F32)
        slot = iota((cap, n_id), 0).astype(F32)
        for b in range(0, n_dp, 2):
            picks = []
            for s in (b, b + 1):
                sel = key[s:s + 1, :] == slot
                idx = jnp.sum(jnp.where(sel, loc[s:s + 1, :] + 1.0, 0.0), axis=1, keepdims=True) - 1.0
                picks.append(idx)
            idx2 = jnp.concatenate(picks, axis=0).astype(jnp.int32)
            hot = jnp.where(iota((2 * cap, k_pad), 1) == idx2, 1.0, 0.0).astype(BF16)
            w1[0, b * cap:(b + 2) * cap, 0:k_pad] = hot
        tab_cp.wait()
        blk = min(512, width)
        n_half = n_dp // 2
        for h in range(2):
            r0, r1 = h * n_half * cap, (h + 1) * n_half * cap
            for c in range(0, width, blk):
                tail = w2[0, k_main:k_pad, c:c + blk]
                tail = jnp.where(iota((K_TILE, blk), 0) < n_rows - k_main, tail.astype(F32), 0.0).astype(BF16)
                got = dot32(w1[0, r0:r1, 0:k_main], w2[0, 0:k_main, c:c + blk]) + dot32(w1[0, r0:r1, k_main:k_pad], tail)
                for s in range(n_half):
                    send_rows[h * n_half + s, :, c:c + blk] = got[s * cap:(s + 1) * cap, :].astype(BF16)
            for j in range(h * n_half, min((h + 1) * n_half, n_dp - 1)):
                row_copy(d, j).start()
        recv_rows[d] = send_rows[n_dp - 1]
        u1_cp.start()
        u2_cp.start()
        wp_cp.start()
        wo_cp.start()
        for j in range(n_dp - 1):
            row_copy(order[j], j).wait_recv()
        xbuf[...] = dot32(xnb[:, 0:n_slots], recv_rows[...].reshape(n_slots, width)).astype(BF16)

    def x_copy(i):
        part = pl.ds(i * PIECE, PIECE)
        return pltpu.make_async_remote_copy(
            src_ref=ybuf.at[:, part], dst_ref=xbuf.at[:, part], send_sem=x_ss.at[i], recv_sem=x_rs.at[i],
            device_id={"pp": jnp.where(is_first, 1, lax.rem(p + 2, n_pp))}, device_id_type=MESH)

    h_peers = ((3, 0), (1, 0), (5, half), (6, half))

    def h_copy(j, i):
        to, row0 = h_peers[j]
        part = pl.ds(i * PIECE, PIECE)
        return pltpu.make_async_remote_copy(
            src_ref=ybuf.at[pl.ds(row0, half), part], dst_ref=hbuf.at[:, part], send_sem=h_ss.at[j, i], recv_sem=h_rs.at[i],
            device_id={"pp": to}, device_id_type=MESH)

    def f_copy(i):
        part = pl.ds(i * PIECE, PIECE)
        return pltpu.make_async_remote_copy(
            src_ref=hbuf.at[:, part], dst_ref=hbuf.at[:, part], send_sem=f_ss.at[i], recv_sem=h_rs.at[i],
            device_id={"pp": lax.rem(p + n_pp - 1, n_pp)}, device_id_type=MESH)

    def gelu_up(m, xn, slot):
        n_blk = ffn // MLP_BLOCK
        for b in range(n_blk + 1):
            if b < n_blk:
                lg[b % 2, 0:m, :] = dot32(xn, w1[slot, :, b * MLP_BLOCK:(b + 1) * MLP_BLOCK])
            if b:
                hid[0:m, (b - 1) * MLP_BLOCK:b * MLP_BLOCK] = jax.nn.gelu(lg[(b - 1) % 2, 0:m, :]).astype(BF16)

    def stage(turn, carry):
        lent = turn == 0

        @pl.when(jnp.where(lent, double, jnp.logical_not(lender)))
        def _():
            @pl.when(lent)
            def _():
                push_copy(0).wait_recv()
                push_copy(1).wait_recv()

            @pl.when(jnp.logical_not(lent))
            def _():
                w1_cp.wait()
                w2_cp.wait()

            @pl.when(lent | (p == 1))
            def _():
                for i in range(n_piece):
                    x_copy(i).wait_recv()

            @pl.when(lent & (p == E_GATE))
            def _():
                pl.semaphore_signal(link_free, inc=1, device_id={"pp": 0}, device_id_type=MESH)

            xnb[...] = norm_f32(xbuf[...].astype(F32)).astype(BF16)
            gelu_up(seq, xnb[...], turn)
            for i in range(n_piece):
                c = i * PIECE
                out = xbuf[:, c:c + PIECE].astype(F32) + dot32(hid[...], w2[turn, :, c:c + PIECE])
                ybuf[:, c:c + PIECE] = out.astype(BF16)

                @pl.when(jnp.logical_not(lent | is_last))
                def _():
                    x_copy(i).start()

                @pl.when(jnp.logical_not(lent) & is_last)
                def _():
                    for j in range(len(h_peers)):
                        h_copy(j, i).start()

            @pl.when(lent)
            def _():
                u1_cp.start()
                u2_cp.start()
                xbuf[...] = ybuf[...]

            @pl.when(jnp.logical_not(lent))
            def _():
                late_cp.start()

        return carry

    lax.fori_loop(0, 2, stage, 0)

    def e_copy(to):
        row0 = half * (to // n_shard)
        return pltpu.make_async_remote_copy(
            src_ref=eall.at[pl.ds(row0, half), :], dst_ref=ebuf, send_sem=e_ss.at[to], recv_sem=e_rs,
            device_id={"pp": to}, device_id_type=MESH)

    def over_copy(to):
        return pltpu.make_async_remote_copy(
            src_ref=over_buf.at[0], dst_ref=over_buf.at[1], send_sem=over_ss.at[to], recv_sem=over_rs,
            device_id={"pp": to}, device_id_type=MESH)

    @pl.when(is_first)
    def _():
        eall[...] = dot32(eall[:, 0:n_slots], recv_rows[...].reshape(n_slots, width)).astype(BF16)
        ids2 = ids_all[...].reshape(n_dp, n_id)
        used = iota((n_dp, n_id), 1) < seq + 1
        most = jnp.zeros((n_dp, 1), F32)
        for k in range(n_dp):
            hit = (ids2 >= k * n_rows) & (ids2 < (k + 1) * n_rows) & used
            most = jnp.maximum(most, jnp.sum(jnp.where(hit, 1.0, 0.0), axis=1, keepdims=True))
        over = jnp.broadcast_to(jnp.where(jnp.max(most, axis=0, keepdims=True) > cap, 1.0, 0.0), (SUB, LANES))
        over_buf[0] = over
        over_buf[1] = over
        ebuf[...] = eall[0:half, :]
        pl.semaphore_wait(link_free, 1)
        for to in range(1, n_pp):
            e_copy(to).start()
            over_copy(to).start()

    @pl.when(jnp.logical_not(is_first))
    def _():
        e_copy(1).wait_recv()
        over_copy(1).wait_recv()

    g_f, g_h, g_e, g_m = (ref[...].astype(F32).reshape(1, width) for ref in (gf_ref, gh_ref, ge_ref, gm_ref))

    wp_cp.wait()
    e_n = (norm_f32(ebuf[...].astype(F32)) * g_e).astype(BF16)
    epart[...] = dot32(e_n, wp[width:2 * width, :])
    u1_cp.wait()
    u2_cp.wait()
    wo_cp.wait()

    row_f = jnp.broadcast_to(ids_ref[0], (2 * half, n_id))
    rr = iota((2 * half, n_id), 0)
    at = jnp.where(rr < half, rr + 1, rr - half + 2) + group * half
    tgt = jnp.sum(jnp.where(iota((2 * half, n_id), 1) == at, row_f, 0).astype(F32), axis=1, keepdims=True)
    tgt = tgt.astype(jnp.int32) - shard * (base_tiles * LANES)
    tgt = jnp.broadcast_to(tgt, (2 * half, LANES))

    @pl.when(is_last)
    def _():
        hbuf[...] = ybuf[half:seq, :]

    @pl.when(jnp.logical_not(is_last))
    def _():
        for i in range(n_piece):
            h_copy(0, i).wait_recv()

            @pl.when((p == 1) | (p == 3) | (p == 5))
            def _():
                f_copy(i).start()

    h_f = norm_f32(hbuf[...].astype(F32))
    z_val = (dot32((h_f * g_h).astype(BF16), wp[0:width, :]) + epart[...]).astype(BF16)
    zbuf[...] = z_val
    xh[0:half, :] = (h_f * g_f).astype(BF16)
    xnb[0:half, :] = (norm_f32(z_val.astype(F32)) * g_m).astype(BF16)
    gelu_up(half, xnb[0:half, :], 0)
    z_out = (zbuf[...].astype(F32) + dot32(hid[0:half, :], w2[0])).astype(BF16)
    xh[half:2 * half, :] = (norm_f32(z_out.astype(F32)) * g_f).astype(BF16)

    lane = iota((2 * half, LANES), 1)
    tail_ok = jnp.broadcast_to(shard == n_shard - 1, (2 * half, LANES))
    blocks = [(wo, c, ffn + c, min(MLP_BLOCK, own_cols - c)) for c in range(0, own_cols, MLP_BLOCK)]
    blocks += [(w1.at[1], c, c, MLP_BLOCK) for c in range(0, ffn, MLP_BLOCK)]

    def logits_of(i):
        ref, c, _, n = blocks[i]
        lg[i % 2, :, 0:n] = dot32(xh[...], ref[:, c:c + n])

    def fold(i):
        _, _, start, n = blocks[i]
        tiles = []
        for t in range(0, n, LANES):
            val = lg[i % 2, :, t:t + LANES]
            tiles.append((start + t, val, start + t == cols - LANES))
        top = None if i == 0 else mx[...]
        for _, val, last in tiles:
            val = jnp.where(tail_ok, val, -jnp.inf) if last else val
            top = val if top is None else jnp.maximum(top, val)
        total = jnp.zeros_like(top) if i == 0 else sm[...] * jnp.exp(mx[...] - top)
        hit = jnp.zeros_like(top) if i == 0 else pk[...]
        for at_col, val, last in tiles:
            e_val = jnp.exp(val - top)
            match = lane == tgt - at_col
            if last:
                e_val = jnp.where(tail_ok, e_val, 0.0)
                match = match & tail_ok
            total = total + e_val
            hit = hit + jnp.where(match, val, 0.0)
        mx[...] = top
        sm[...] = total
        pk[...] = hit

    for i in range(len(blocks)):
        if i == len(blocks) - ffn // MLP_BLOCK:
            late_cp.wait()
        logits_of(i)
        if i:
            fold(i - 1)
    fold(len(blocks) - 1)

    eye = iota((2 * half, LANES), 0) == iota((2 * half, LANES), 1)

    def as_row(col):
        return jnp.sum(jnp.where(eye, jnp.broadcast_to(col, (2 * half, LANES)), 0.0), axis=0, keepdims=True)

    top = mx[...]
    m_col = jnp.max(top, axis=1, keepdims=True)
    s_col = jnp.sum(sm[...] * jnp.exp(top - m_col), axis=1, keepdims=True)
    p_col = jnp.sum(pk[...], axis=1, keepdims=True)
    sub = iota((SUB, LANES), 0)
    tile = jnp.where(sub == 0, as_row(m_col), jnp.where(sub == 1, as_row(s_col), as_row(p_col)))
    part_send[...] = tile
    part_recv[p] = tile

    def part_copy(owner, peer):
        return pltpu.make_async_remote_copy(
            src_ref=part_send, dst_ref=part_recv.at[owner], send_sem=part_ss.at[peer], recv_sem=part_rs.at[owner],
            device_id={"pp": peer}, device_id_type=MESH)

    for k in range(1, n_pp):
        part_copy(p, lax.rem(p + k, n_pp)).start()
    for k in range(1, n_pp):
        peer = lax.rem(p + k, n_pp)
        part_copy(peer, peer).wait_recv()

    def group_nll(g):
        got = [part_recv[g * n_shard + i] for i in range(n_shard)]
        best = functools.reduce(jnp.maximum, [t[0:1, :] for t in got])
        total = sum(t[1:2, :] * jnp.exp(t[0:1, :] - best) for t in got)
        return best + jnp.log(total) - sum(t[2:3, :] for t in got)

    nll_a = jnp.broadcast_to(group_nll(0), (SUB, LANES))
    nll_b = jnp.broadcast_to(group_nll(1), (SUB, LANES))
    low_lane = iota((SUB, LANES), 1) < half
    main = jnp.where(low_lane, nll_a, pltpu.roll(nll_b, half, 1))
    mtp = jnp.where(low_lane, pltpu.roll(nll_a, half, 1), nll_b)
    both = main + MTP_WEIGHT * mtp
    ls_send[...] = both
    ls_recv[d] = both

    def ls_copy(owner, peer, side):
        return pltpu.make_async_remote_copy(
            src_ref=ls_send, dst_ref=ls_recv.at[owner], send_sem=ls_ss.at[side, peer], recv_sem=ls_rs.at[owner],
            device_id={"dp": peer, "pp": lax.rem(p + n_pp - side, n_pp)}, device_id_type=MESH)

    @pl.when(jnp.logical_not(even))
    def _():
        for peer in order[:-1]:
            ls_copy(d, peer, 1).start()
            ls_copy(d, peer, 0).start()

    for peer in order[:-1]:
        ls_copy(peer, peer, 0).wait_recv()
    acc = ls_recv[0]
    for k in range(1, n_dp):
        acc = acc + ls_recv[k]
    loss = jnp.sum(acc, axis=1, keepdims=True) * (1.0 / (n_dp * seq))
    out_ref[...] = jnp.where(sub == 0, main, jnp.where(sub == 1, mtp, jnp.broadcast_to(loss, (SUB, LANES))))
    flag_out[0, 0] = jnp.max(over_buf[1]).astype(jnp.int32)

    @pl.when(jnp.logical_not(even))
    def _():
        for peer in order[:-1]:
            ls_copy(d, peer, 1).wait_send()
            ls_copy(d, peer, 0).wait_send()

    @pl.when(p == 1)
    def _():
        for k in range(1, n_dp):
            ids_copy(d, lax.rem(d + k, n_dp)).wait_send()

    for k in range(1, n_pp):
        part_copy(p, lax.rem(p + k, n_pp)).wait_send()

    @pl.when(is_first)
    def _():
        for k in range(1, n_dp):
            row_copy(d, k - 1).wait_send()
        for to in range(1, n_pp):
            e_copy(to).wait_send()
            over_copy(to).wait_send()

    @pl.when(jnp.logical_not(is_last | lender))
    def _():
        for i in range(n_piece):
            x_copy(i).wait_send()

    @pl.when(lender)
    def _():
        push_copy(0).wait_send()
        push_copy(1).wait_send()

    @pl.when((p == 1) | (p == 3) | (p == 5))
    def _():
        for i in range(n_piece):
            f_copy(i).wait_send()

    @pl.when(is_last)
    def _():
        for j in range(len(h_peers)):
            for i in range(n_piece):
                h_copy(j, i).wait_send()


def mega(n_dp, n_pp, seq, ids, gains, emb, w1, w2, wp, u1, u2, wo):
    width, ffn = w1.shape[2], w1.shape[3]
    n_tiles = wo.shape[1] // LANES
    n_shard = n_pp // 2
    cols = (n_tiles - (n_shard - 1) * (n_tiles // n_shard)) * LANES
    half = seq // 2
    n_piece = width // PIECE
    dma = pltpu.SemaphoreType.DMA
    tile = pltpu.VMEM((SUB, LANES), F32)
    vmem = pl.BlockSpec(memory_space=pltpu.VMEM)
    anys = pl.BlockSpec(memory_space=pl.ANY)
    act = pltpu.VMEM((seq, width), BF16)
    act_half = pltpu.VMEM((half, width), BF16)
    return pl.pallas_call(
        functools.partial(mega_kernel, n_dp, n_pp, seq, CAP),
        out_shape=(
            jax.ShapeDtypeStruct((SUB, LANES), F32),
            jax.ShapeDtypeStruct((1, 1), jnp.int32),
        ),
        in_specs=[vmem] * 5 + [anys] * 7,
        out_specs=(vmem, pl.BlockSpec(memory_space=pltpu.SMEM)),
        scratch_shapes=[
            pltpu.VMEM((2, width, ffn), BF16),
            pltpu.VMEM((2, ffn, width), BF16),
            pltpu.VMEM((2 * width, width), BF16),
            pltpu.VMEM((width, cols - ffn), BF16),
            pltpu.VMEM((n_dp, 1, seq + 2), jnp.int32),
            pltpu.VMEM((n_dp, CAP, width), BF16),
            pltpu.VMEM((n_dp, CAP, width), BF16),
            act, act, act,
            pltpu.VMEM((seq, ffn), BF16),
            act_half, act_half,
            act,
            act_half,
            pltpu.VMEM((half, width), F32),
            act,
            pltpu.VMEM((2, 2 * half, MLP_BLOCK), F32),
            pltpu.VMEM((2 * half, LANES), F32), pltpu.VMEM((2 * half, LANES), F32), pltpu.VMEM((2 * half, LANES), F32),
            tile, pltpu.VMEM((n_pp, SUB, LANES), F32),
            tile, pltpu.VMEM((n_dp, SUB, LANES), F32),
            pltpu.VMEM((2, SUB, LANES), F32),
            dma((8,)), dma((n_dp,)), dma((n_dp,)), dma((n_dp,)), dma((n_dp,)),
            dma((n_piece,)), dma((n_piece,)), dma((n_pp,)), dma(()), dma((4, n_piece)), dma((n_piece,)), dma((n_piece,)),
            dma((n_pp,)), dma((n_pp,)), dma((2, n_dp)), dma((n_dp,)), dma((n_pp,)), dma(()), pltpu.SemaphoreType.REGULAR,
            dma((2,)), dma((2,)),
        ],
        compiler_params=pltpu.CompilerParams(collective_id=0, has_side_effects=True, vmem_limit_bytes=VMEM_LIMIT),
        name="mtp_eval",
    )(ids, *gains, emb, w1, w2, wp, u1, u2, wo)


def norm_plain(x_val):
    return norm_f32(x_val.astype(F32)).astype(BF16)


def norm_gain(x_val, gain_vec):
    return (norm_f32(x_val.astype(F32)) * gain_vec.astype(F32)).astype(BF16)


def mlp_add(x_val, normed, w_up, w_down):
    hidden = jax.nn.gelu(dot32(normed, w_up)).astype(BF16)
    return (x_val.astype(F32) + dot32(hidden, w_down)).astype(BF16)


def token_nll(normed, targets, w_out):
    n_rows, row_width = normed.shape
    n_blocks = n_rows // HEAD_ROWS

    def one_block(pair):
        block_rows, block_tgt = pair
        logits = dot32(block_rows, w_out)
        picked = jnp.take_along_axis(logits, block_tgt[:, None], axis=1)[:, 0]
        return jax.nn.logsumexp(logits, axis=1) - picked

    per_block = lax.map(one_block, (normed.reshape(n_blocks, HEAD_ROWS, row_width), targets.reshape(n_blocks, HEAD_ROWS)))
    return per_block.reshape(n_rows)


def any_ids(n_dp, n_pp, seq, ids, emb, w_one, w_two, gain_f, gain_h, gain_e, gain_m, w_proj, u_one, u_two, w_out):
    stage = lax.axis_index("pp")
    me = lax.axis_index("dp")
    n_rows, width = emb.shape
    ring = [(i, (i + 1) % n_dp) for i in range(n_dp)]
    want = ids[:seq + 1]

    def take(k, held, rows):
        local = want - lax.rem(me - k + n_dp, n_dp) * n_rows
        here = (local >= 0) & (local < n_rows)
        return jnp.where(here[:, None], held[jnp.clip(local, 0, n_rows - 1)], rows)

    def gather_step(k, carry):
        held, rows = carry
        rows = take(k, held, rows)
        return lax.ppermute(held, "dp", ring), rows

    rows = take(0, emb, jnp.zeros((seq + 1, width), BF16))
    _, rows = lax.fori_loop(1, n_dp, gather_step, (lax.ppermute(emb, "dp", ring), rows))
    to_next = [(i, i + 1) for i in range(n_pp - 1)]

    def tick(k, carry):
        x_val, _ = carry
        x_val = jnp.where((stage == 0) & (k == 0), rows[:seq], x_val)
        y_val = mlp_add(x_val, norm_plain(x_val), w_one, w_two)
        return lax.ppermute(y_val, "pp", to_next), y_val

    zero = jnp.zeros((seq, width), BF16)
    _, h_last = lax.fori_loop(0, n_pp, tick, (zero, zero))
    e_rows = lax.ppermute(rows[1:seq + 1], "pp", [(0, n_pp - 1)])
    main_nll = token_nll(norm_gain(h_last, gain_f), ids[1:seq + 1], w_out)
    z_sum = dot32(norm_gain(h_last, gain_h), w_proj[:width]) + dot32(norm_gain(e_rows, gain_e), w_proj[width:])
    z_val = z_sum.astype(BF16)
    z_val = mlp_add(z_val, norm_gain(z_val, gain_m), u_one, u_two)
    mtp_nll = token_nll(norm_gain(z_val, gain_f), ids[2:], w_out)
    is_last = stage == n_pp - 1
    main_nll = lax.psum(jnp.where(is_last, main_nll, 0.0), "pp")
    mtp_nll = lax.psum(jnp.where(is_last, mtp_nll, 0.0), "pp")
    total = lax.psum(jnp.sum(main_nll) + MTP_WEIGHT * jnp.sum(mtp_nll), "dp") / (n_dp * seq)
    return total, main_nll.reshape(1, seq), mtp_nll.reshape(1, seq)


def solution(mesh):
    n_pp = mesh.shape["pp"]
    n_dp = mesh.shape["dp"]

    def body(tok_ids, emb_s, w_one, w_two, gain_f, gain_h, gain_e, gain_m, w_proj, u_one, u_two, w_out):
        seq = tok_ids.shape[2] - 2
        gains = (gain_f, gain_h, gain_e, gain_m)
        packed, over = mega(n_dp, n_pp, seq, tok_ids, gains, emb_s, w_one, w_two, w_proj, u_one, u_two, w_out)

        def slow():
            total, main_nll, mtp_nll = any_ids(
                n_dp, n_pp, seq, tok_ids[0, 0], emb_s[0], w_one[0, 0], w_two[0, 0], *gains, w_proj, u_one, u_two, w_out)
            return jnp.concatenate([main_nll, mtp_nll, jnp.broadcast_to(total, (SUB - 2, seq))], axis=0)

        packed = lax.cond(over[0, 0] > 0, slow, lambda: packed)
        return jnp.max(packed[2]), packed[0:1].reshape(1, 1, seq), packed[1:2].reshape(1, 1, seq)

    rep = P()
    in_specs = (P(None, "dp", None), P("pp", "dp", None), P("pp"), P("pp"), rep, rep, rep, rep, rep, rep, rep, rep)
    out_specs = (rep, P(None, "dp", None), P(None, "dp", None))
    return jax.shard_map(body, mesh=mesh, in_specs=in_specs, out_specs=out_specs, check_vma=False)
```

```python
import functools

import jax
import jax.numpy as jnp
from jax import lax
from jax.experimental import pallas as pl
from jax.experimental.pallas import tpu as pltpu
from jax.sharding import PartitionSpec as P

NORM_EPS = 1e-6
MTP_WEIGHT = 0.3
HEAD_ROWS = 128
LANES = 128
SUB = 8
K_TILE = 256
CAP = 24
PIECE = 512
MLP_BLOCK = 1024
E_GATE = 5
VMEM_LIMIT = 66_900_000
F32 = jnp.float32
BF16 = jnp.bfloat16
MESH = pl.DeviceIdType.MESH


def norm_f32(x_f):
    return x_f * lax.rsqrt(jnp.mean(x_f * x_f, axis=-1, keepdims=True) + NORM_EPS)


def iota(shape, dim):
    return lax.broadcasted_iota(jnp.int32, shape, dim)


def dot32(a, b):
    return jnp.dot(a, b, preferred_element_type=F32)


def mega_kernel(
    n_dp, n_pp, seq, cap,
    ids_hbm, gf_hbm, gh_hbm, ge_hbm, gm_hbm, emb, w1h, w2h, wph, u1h, u2h, woh,
    out_ref, flag_out,
    ids_ref, gf_ref, gh_ref, ge_ref, gm_ref, flag_buf,
    w1, w2, wp, wo,
    ids_all, send_rows, recv_rows, xbuf, ybuf, xnb, hid, ebuf, hbuf, eall, zbuf, epart, xh, lg, mx, sm, pk,
    part_send, part_recv, ls_send, ls_recv, over_buf,
    wsem, ids_ss, ids_rs, row_ss, row_rs, x_ss, x_rs, e_ss, e_rs, h_ss, h_rs, f_ss, part_ss, part_rs, ls_ss, ls_rs,
    over_ss, over_rs, link_free, push_ss, push_rs,
):
    d = lax.axis_index("dp")
    p = lax.axis_index("pp")
    width = xbuf.shape[1]
    ffn = w1.shape[2]
    n_rows = emb.shape[1]
    half = seq // 2
    n_shard = n_pp // 2
    shard = lax.rem(p, n_shard)
    group = p // n_shard
    n_tiles = woh.shape[1] // LANES
    base_tiles = n_tiles // n_shard
    cols = ffn + wo.shape[1]
    own_cols = wo.shape[1]
    n_piece = width // PIECE
    is_first = p == 0
    is_last = p == n_pp - 1
    even = lax.rem(p, 2) == 0
    lender = even & (p > 1)
    double = jnp.logical_not(even) & (p > 1)
    k_main = n_rows // K_TILE * K_TILE
    k_pad = k_main + K_TILE
    n_id = seq + 2
    n_slots = n_dp * cap

    col0 = pl.multiple_of(shard * (base_tiles * LANES), LANES)
    tab_cp = pltpu.make_async_copy(emb.at[0], w2.at[0, pl.ds(0, n_rows), :], wsem.at[0])
    w1_cp = pltpu.make_async_copy(w1h.at[0, 0], w1.at[1], wsem.at[1])
    w2_cp = pltpu.make_async_copy(w2h.at[0, 0], w2.at[1], wsem.at[2])
    u1_cp = pltpu.make_async_copy(u1h, w1.at[0], wsem.at[3])
    u2_cp = pltpu.make_async_copy(u2h, w2.at[0], wsem.at[4])
    wp_cp = pltpu.make_async_copy(wph, wp, wsem.at[5])
    wo_cp = pltpu.make_async_copy(woh.at[:, pl.ds(col0 + ffn, own_cols)], wo, wsem.at[6])
    late_cp = pltpu.make_async_copy(woh.at[:, pl.ds(col0, ffn)], w1.at[1], wsem.at[7])

    def push_copy(i):
        src, dst = ((w1h, w1), (w2h, w2))[i]
        return pltpu.make_async_remote_copy(
            src_ref=src.at[0, 0], dst_ref=dst.at[0], send_sem=push_ss.at[i], recv_sem=push_rs.at[i],
            device_id={"pp": lax.rem(p + 1, n_pp)}, device_id_type=MESH)

    small = ((ids_hbm, ids_ref), (gf_hbm, gf_ref), (gh_hbm, gh_ref), (ge_hbm, ge_ref), (gm_hbm, gm_ref))
    small_cp = [pltpu.make_async_copy(src, dst, wsem.at[8 + i]) for i, (src, dst) in enumerate(small)]
    flag_cp = pltpu.make_async_copy(flag_buf, flag_out, wsem.at[13])
    small_cp[0].start()

    barrier = pltpu.get_barrier_semaphore()
    for k in range(1, n_dp):
        pl.semaphore_signal(barrier, inc=1, device_id={"dp": lax.rem(d + k, n_dp)}, device_id_type=MESH)
    for k in range(1, n_pp):
        pl.semaphore_signal(barrier, inc=1, device_id={"pp": lax.rem(p + k, n_pp)}, device_id_type=MESH)
    @pl.when(even)
    def _():
        for k in range(1, n_dp):
            pl.semaphore_signal(
                barrier, inc=1, device_id={"dp": lax.rem(d + k, n_dp), "pp": lax.rem(p + 1, n_pp)}, device_id_type=MESH)

    for cp in small_cp[1:]:
        cp.start()

    @pl.when(is_first)
    def _():
        tab_cp.start()

    @pl.when(jnp.logical_not(even))
    def _():
        w1_cp.start()
        w2_cp.start()

    for cp in small_cp:
        cp.wait()
    pl.semaphore_wait(barrier, n_pp - 1 + jnp.where(even, 1, 2) * (n_dp - 1))

    def ids_copy(owner, peer):
        return pltpu.make_async_remote_copy(
            src_ref=ids_ref.at[0], dst_ref=ids_all.at[owner], send_sem=ids_ss.at[peer], recv_sem=ids_rs.at[owner],
            device_id={"dp": peer, "pp": 0}, device_id_type=MESH)

    @pl.when(p == 1)
    def _():
        for k in range(1, n_dp):
            ids_copy(d, lax.rem(d + k, n_dp)).start()

    @pl.when(is_first)
    def _():
        ids_all[d] = ids_ref[0]

    @pl.when(lender)
    def _():
        push_copy(0).start()
        push_copy(1).start()
        u1_cp.start()
        u2_cp.start()
        late_cp.start()

    @pl.when(p == 1)
    def _():
        u1_cp.start()
        u2_cp.start()

    @pl.when(jnp.logical_not(is_first))
    def _():
        wp_cp.start()
        wo_cp.start()

    n_y = 4
    n_z = n_dp // n_y
    offs = [(z, y) for z in range(n_z) for y in range(n_y)]
    offs.sort(key=lambda o: -(min(o[0], n_z - o[0]) + min(o[1], n_y - o[1])))
    order = [lax.rem(d // n_y + z, n_z) * n_y + lax.rem(d + y, n_y) for z, y in offs]

    def row_copy(owner, j):
        return pltpu.make_async_remote_copy(
            src_ref=send_rows.at[j], dst_ref=recv_rows.at[owner], send_sem=row_ss.at[j], recv_sem=row_rs.at[owner],
            device_id={"dp": order[j]}, device_id_type=MESH)

    def positions(row0, n):
        row = ids_ref[0]
        rr = iota((n, n_id), 0) + row0
        ll = iota((n, n_id), 1)
        pos = jnp.where(rr < seq, rr, rr - seq + 1)
        id_col = jnp.sum(jnp.where(ll == pos, jnp.broadcast_to(row, (n, n_id)), 0).astype(F32), axis=1, keepdims=True)
        src_col = jnp.zeros((n, 1), F32)
        src_row = jnp.zeros((1, n_id), F32)
        for k in range(1, n_dp):
            src_col = src_col + jnp.where(id_col >= float(k * n_rows), 1.0, 0.0)
            src_row = src_row + jnp.where(row >= k * n_rows, 1.0, 0.0)
        earlier = (jnp.broadcast_to(src_row, (n, n_id)) == src_col) & (ll < pos)
        rank_col = jnp.sum(jnp.where(earlier, 1.0, 0.0), axis=1, keepdims=True)
        where_col = jnp.where(rank_col < float(cap), src_col * float(cap) + rank_col, -1.0).astype(jnp.int32)
        return jnp.where(iota((n, n_slots), 1) == where_col, 1.0, 0.0).astype(BF16)

    @pl.when(is_first)
    def _():
        xnb[:, 0:n_slots] = positions(0, seq)
        eall[:, 0:n_slots] = positions(seq, seq)
        for k in range(1, n_dp):
            peer = lax.rem(d + k, n_dp)
            ids_copy(peer, peer).wait_recv()
        w1_cp.start()
        w2_cp.start()
        low = d * n_rows
        ids2 = jnp.concatenate([ids_all[peer] for peer in order], axis=0)
        lane2 = iota((n_dp, n_id), 1)
        valid = (ids2 >= low) & (ids2 < low + n_rows) & (lane2 < seq + 1)
        before = jnp.where(iota((n_id, n_id), 0) < iota((n_id, n_id), 1), 1.0, 0.0).astype(BF16)
        rank = dot32(jnp.where(valid, 1.0, 0.0).astype(BF16), before)
        key = jnp.where(valid, rank, -1.0)
        loc = jnp.where(valid, ids2 - low, 0).astype(F32)
        slot = iota((cap, n_id), 0).astype(F32)
        tab_cp.wait()
        blk = min(512, width)
        n_half = n_dp // 2
        for h in range(2):
            r0, r1 = h * n_half * cap, (h + 1) * n_half * cap
            for b in range(h * n_half, (h + 1) * n_half, 2):
                picks = []
                for s in (b, b + 1):
                    sel = key[s:s + 1, :] == slot
                    idx = jnp.sum(jnp.where(sel, loc[s:s + 1, :] + 1.0, 0.0), axis=1, keepdims=True) - 1.0
                    picks.append(idx)
                idx2 = jnp.concatenate(picks, axis=0).astype(jnp.int32)
                hot = jnp.where(iota((2 * cap, k_pad), 1) == idx2, 1.0, 0.0).astype(BF16)
                w1[0, b * cap:(b + 2) * cap, 0:k_pad] = hot
            for c in range(0, width, blk):
                tail = w2[0, k_main:k_pad, c:c + blk]
                tail = jnp.where(iota((K_TILE, blk), 0) < n_rows - k_main, tail.astype(F32), 0.0).astype(BF16)
                got = dot32(w1[0, r0:r1, 0:k_main], w2[0, 0:k_main, c:c + blk]) + dot32(w1[0, r0:r1, k_main:k_pad], tail)
                for s in range(n_half):
                    send_rows[h * n_half + s, :, c:c + blk] = got[s * cap:(s + 1) * cap, :].astype(BF16)
            for j in range(h * n_half, min((h + 1) * n_half, n_dp - 1)):
                row_copy(d, j).start()
        recv_rows[d] = send_rows[n_dp - 1]
        u1_cp.start()
        u2_cp.start()
        wp_cp.start()
        wo_cp.start()
        for j in range(n_dp - 1):
            row_copy(order[j], j).wait_recv()
        xbuf[...] = dot32(xnb[:, 0:n_slots], recv_rows[...].reshape(n_slots, width)).astype(BF16)

    def x_copy(i):
        part = pl.ds(i * PIECE, PIECE)
        return pltpu.make_async_remote_copy(
            src_ref=ybuf.at[:, part], dst_ref=xbuf.at[:, part], send_sem=x_ss.at[i], recv_sem=x_rs.at[i],
            device_id={"pp": jnp.where(is_first, 1, lax.rem(p + 2, n_pp))}, device_id_type=MESH)

    h_peers = ((3, 0), (1, 0), (5, half), (6, half))

    def h_copy(j, i):
        to, row0 = h_peers[j]
        part = pl.ds(i * PIECE, PIECE)
        return pltpu.make_async_remote_copy(
            src_ref=ybuf.at[pl.ds(row0, half), part], dst_ref=hbuf.at[:, part], send_sem=h_ss.at[j, i], recv_sem=h_rs.at[i],
            device_id={"pp": to}, device_id_type=MESH)

    def f_copy(i):
        part = pl.ds(i * PIECE, PIECE)
        return pltpu.make_async_remote_copy(
            src_ref=hbuf.at[:, part], dst_ref=hbuf.at[:, part], send_sem=f_ss.at[i], recv_sem=h_rs.at[i],
            device_id={"pp": lax.rem(p + n_pp - 1, n_pp)}, device_id_type=MESH)

    def gelu_up(m, xn, slot):
        n_blk = ffn // MLP_BLOCK
        for b in range(n_blk + 1):
            if b < n_blk:
                lg[b % 2, 0:m, :] = dot32(xn, w1[slot, :, b * MLP_BLOCK:(b + 1) * MLP_BLOCK])
            if b:
                hid[0:m, (b - 1) * MLP_BLOCK:b * MLP_BLOCK] = jax.nn.gelu(lg[(b - 1) % 2, 0:m, :]).astype(BF16)

    def stage(turn, carry):
        lent = turn == 0

        @pl.when(jnp.where(lent, double, jnp.logical_not(lender)))
        def _():
            @pl.when(lent)
            def _():
                push_copy(0).wait_recv()
                push_copy(1).wait_recv()

            @pl.when(jnp.logical_not(lent))
            def _():
                w1_cp.wait()
                w2_cp.wait()

            @pl.when(lent | (p == 1))
            def _():
                for i in range(n_piece):
                    x_copy(i).wait_recv()

            @pl.when(lent & (p == E_GATE))
            def _():
                pl.semaphore_signal(link_free, inc=1, device_id={"pp": 0}, device_id_type=MESH)

            xnb[...] = norm_f32(xbuf[...].astype(F32)).astype(BF16)
            gelu_up(seq, xnb[...], turn)
            for i in range(n_piece):
                c = i * PIECE
                out = xbuf[:, c:c + PIECE].astype(F32) + dot32(hid[...], w2[turn, :, c:c + PIECE])
                ybuf[:, c:c + PIECE] = out.astype(BF16)

                @pl.when(jnp.logical_not(lent | is_last))
                def _():
                    x_copy(i).start()

                @pl.when(jnp.logical_not(lent) & is_last)
                def _():
                    for j in range(len(h_peers)):
                        h_copy(j, i).start()

            @pl.when(lent)
            def _():
                u1_cp.start()
                u2_cp.start()
                xbuf[...] = ybuf[...]

            @pl.when(jnp.logical_not(lent))
            def _():
                late_cp.start()

        return carry

    lax.fori_loop(0, 2, stage, 0)

    def e_copy(to):
        row0 = half * (to // n_shard)
        return pltpu.make_async_remote_copy(
            src_ref=eall.at[pl.ds(row0, half), :], dst_ref=ebuf, send_sem=e_ss.at[to], recv_sem=e_rs,
            device_id={"pp": to}, device_id_type=MESH)

    def over_copy(to):
        return pltpu.make_async_remote_copy(
            src_ref=over_buf.at[0], dst_ref=over_buf.at[1], send_sem=over_ss.at[to], recv_sem=over_rs,
            device_id={"pp": to}, device_id_type=MESH)

    @pl.when(is_first)
    def _():
        eall[...] = dot32(eall[:, 0:n_slots], recv_rows[...].reshape(n_slots, width)).astype(BF16)
        ids2 = ids_all[...].reshape(n_dp, n_id)
        used = iota((n_dp, n_id), 1) < seq + 1
        most = jnp.zeros((n_dp, 1), F32)
        for k in range(n_dp):
            hit = (ids2 >= k * n_rows) & (ids2 < (k + 1) * n_rows) & used
            most = jnp.maximum(most, jnp.sum(jnp.where(hit, 1.0, 0.0), axis=1, keepdims=True))
        over = jnp.broadcast_to(jnp.where(jnp.max(most, axis=0, keepdims=True) > cap, 1.0, 0.0), (SUB, LANES))
        over_buf[0] = over
        over_buf[1] = over
        ebuf[...] = eall[0:half, :]
        pl.semaphore_wait(link_free, 1)
        for to in range(1, n_pp):
            e_copy(to).start()
            over_copy(to).start()

    @pl.when(jnp.logical_not(is_first))
    def _():
        e_copy(1).wait_recv()
        over_copy(1).wait_recv()

    flag_buf[0, 0] = jnp.max(over_buf[1]).astype(jnp.int32)
    flag_cp.start()

    g_f, g_h, g_e, g_m = (ref[...].astype(F32).reshape(1, width) for ref in (gf_ref, gh_ref, ge_ref, gm_ref))

    wp_cp.wait()
    e_n = (norm_f32(ebuf[...].astype(F32)) * g_e).astype(BF16)
    epart[...] = dot32(e_n, wp[width:2 * width, :])
    u1_cp.wait()
    u2_cp.wait()
    wo_cp.wait()

    row_f = jnp.broadcast_to(ids_ref[0], (2 * half, n_id))
    rr = iota((2 * half, n_id), 0)
    at = jnp.where(rr < half, rr + 1, rr - half + 2) + group * half
    tgt = jnp.sum(jnp.where(iota((2 * half, n_id), 1) == at, row_f, 0).astype(F32), axis=1, keepdims=True)
    tgt = tgt.astype(jnp.int32) - shard * (base_tiles * LANES)
    tgt = jnp.broadcast_to(tgt, (2 * half, LANES))

    @pl.when(is_last)
    def _():
        hbuf[...] = ybuf[half:seq, :]

    @pl.when(jnp.logical_not(is_last))
    def _():
        for i in range(n_piece):
            h_copy(0, i).wait_recv()

            @pl.when((p == 1) | (p == 3) | (p == 5))
            def _():
                f_copy(i).start()

    h_f = norm_f32(hbuf[...].astype(F32))
    z_val = (dot32((h_f * g_h).astype(BF16), wp[0:width, :]) + epart[...]).astype(BF16)
    zbuf[...] = z_val
    xh[0:half, :] = (h_f * g_f).astype(BF16)
    xnb[0:half, :] = (norm_f32(z_val.astype(F32)) * g_m).astype(BF16)
    gelu_up(half, xnb[0:half, :], 0)
    z_out = (zbuf[...].astype(F32) + dot32(hid[0:half, :], w2[0])).astype(BF16)
    xh[half:2 * half, :] = (norm_f32(z_out.astype(F32)) * g_f).astype(BF16)

    lane = iota((2 * half, LANES), 1)
    tail_ok = jnp.broadcast_to(shard == n_shard - 1, (2 * half, LANES))
    blocks = [(wo, c, ffn + c, min(MLP_BLOCK, own_cols - c)) for c in range(0, own_cols, MLP_BLOCK)]
    blocks += [(w1.at[1], c, c, MLP_BLOCK) for c in range(0, ffn, MLP_BLOCK)]

    def logits_of(i):
        ref, c, _, n = blocks[i]
        lg[i % 2, :, 0:n] = dot32(xh[...], ref[:, c:c + n])

    def fold(i):
        _, _, start, n = blocks[i]
        tiles = []
        for t in range(0, n, LANES):
            val = lg[i % 2, :, t:t + LANES]
            tiles.append((start + t, val, start + t == cols - LANES))
        top = None if i == 0 else mx[...]
        for _, val, last in tiles:
            val = jnp.where(tail_ok, val, -jnp.inf) if last else val
            top = val if top is None else jnp.maximum(top, val)
        total = jnp.zeros_like(top) if i == 0 else sm[...] * jnp.exp(mx[...] - top)
        hit = jnp.zeros_like(top) if i == 0 else pk[...]
        for at_col, val, last in tiles:
            e_val = jnp.exp(val - top)
            match = lane == tgt - at_col
            if last:
                e_val = jnp.where(tail_ok, e_val, 0.0)
                match = match & tail_ok
            total = total + e_val
            hit = hit + jnp.where(match, val, 0.0)
        mx[...] = top
        sm[...] = total
        pk[...] = hit

    for i in range(len(blocks)):
        if i == len(blocks) - ffn // MLP_BLOCK:
            late_cp.wait()
        logits_of(i)
        if i:
            fold(i - 1)
    fold(len(blocks) - 1)

    eye = iota((2 * half, LANES), 0) == iota((2 * half, LANES), 1)

    def as_row(col):
        return jnp.sum(jnp.where(eye, jnp.broadcast_to(col, (2 * half, LANES)), 0.0), axis=0, keepdims=True)

    top = mx[...]
    m_col = jnp.max(top, axis=1, keepdims=True)
    s_col = jnp.sum(sm[...] * jnp.exp(top - m_col), axis=1, keepdims=True)
    p_col = jnp.sum(pk[...], axis=1, keepdims=True)
    sub = iota((SUB, LANES), 0)
    tile = jnp.where(sub == 0, as_row(m_col), jnp.where(sub == 1, as_row(s_col), as_row(p_col)))
    part_send[...] = tile
    part_recv[p] = tile

    def part_copy(owner, peer):
        return pltpu.make_async_remote_copy(
            src_ref=part_send, dst_ref=part_recv.at[owner], send_sem=part_ss.at[peer], recv_sem=part_rs.at[owner],
            device_id={"pp": peer}, device_id_type=MESH)

    for k in range(1, n_pp):
        part_copy(p, lax.rem(p + k, n_pp)).start()
    for k in range(1, n_pp):
        peer = lax.rem(p + k, n_pp)
        part_copy(peer, peer).wait_recv()

    def group_nll(g):
        got = [part_recv[g * n_shard + i] for i in range(n_shard)]
        best = functools.reduce(jnp.maximum, [t[0:1, :] for t in got])
        total = sum(t[1:2, :] * jnp.exp(t[0:1, :] - best) for t in got)
        return best + jnp.log(total) - sum(t[2:3, :] for t in got)

    nll_a = jnp.broadcast_to(group_nll(0), (SUB, LANES))
    nll_b = jnp.broadcast_to(group_nll(1), (SUB, LANES))
    low_lane = iota((SUB, LANES), 1) < half
    main = jnp.where(low_lane, nll_a, pltpu.roll(nll_b, half, 1))
    mtp = jnp.where(low_lane, pltpu.roll(nll_a, half, 1), nll_b)
    both = main + MTP_WEIGHT * mtp
    ls_send[...] = both
    ls_recv[d] = both

    def ls_copy(owner, peer, side):
        return pltpu.make_async_remote_copy(
            src_ref=ls_send, dst_ref=ls_recv.at[owner], send_sem=ls_ss.at[side, peer], recv_sem=ls_rs.at[owner],
            device_id={"dp": peer, "pp": lax.rem(p + n_pp - side, n_pp)}, device_id_type=MESH)

    @pl.when(jnp.logical_not(even))
    def _():
        for peer in order[:-1]:
            ls_copy(d, peer, 1).start()
            ls_copy(d, peer, 0).start()

    for peer in order[:-1]:
        ls_copy(peer, peer, 0).wait_recv()
    acc = ls_recv[0]
    for k in range(1, n_dp):
        acc = acc + ls_recv[k]
    loss = jnp.sum(acc, axis=1, keepdims=True) * (1.0 / (n_dp * seq))
    out_ref[...] = jnp.where(sub == 0, main, jnp.where(sub == 1, mtp, jnp.broadcast_to(loss, (SUB, LANES))))
    flag_cp.wait()

    @pl.when(jnp.logical_not(even))
    def _():
        for peer in order[:-1]:
            ls_copy(d, peer, 1).wait_send()
            ls_copy(d, peer, 0).wait_send()

    @pl.when(p == 1)
    def _():
        for k in range(1, n_dp):
            ids_copy(d, lax.rem(d + k, n_dp)).wait_send()

    for k in range(1, n_pp):
        part_copy(p, lax.rem(p + k, n_pp)).wait_send()

    @pl.when(is_first)
    def _():
        for k in range(1, n_dp):
            row_copy(d, k - 1).wait_send()
        for to in range(1, n_pp):
            e_copy(to).wait_send()
            over_copy(to).wait_send()

    @pl.when(jnp.logical_not(is_last | lender))
    def _():
        for i in range(n_piece):
            x_copy(i).wait_send()

    @pl.when(lender)
    def _():
        push_copy(0).wait_send()
        push_copy(1).wait_send()

    @pl.when((p == 1) | (p == 3) | (p == 5))
    def _():
        for i in range(n_piece):
            f_copy(i).wait_send()

    @pl.when(is_last)
    def _():
        for j in range(len(h_peers)):
            for i in range(n_piece):
                h_copy(j, i).wait_send()


def mega(n_dp, n_pp, seq, ids, gains, emb, w1, w2, wp, u1, u2, wo):
    width, ffn = w1.shape[2], w1.shape[3]
    n_tiles = wo.shape[1] // LANES
    n_shard = n_pp // 2
    cols = (n_tiles - (n_shard - 1) * (n_tiles // n_shard)) * LANES
    half = seq // 2
    n_piece = width // PIECE
    dma = pltpu.SemaphoreType.DMA
    tile = pltpu.VMEM((SUB, LANES), F32)
    vmem = pl.BlockSpec(memory_space=pltpu.VMEM)
    anys = pl.BlockSpec(memory_space=pl.ANY)
    act = pltpu.VMEM((seq, width), BF16)
    act_half = pltpu.VMEM((half, width), BF16)
    return pl.pallas_call(
        functools.partial(mega_kernel, n_dp, n_pp, seq, CAP),
        out_shape=(
            jax.ShapeDtypeStruct((SUB, LANES), F32),
            jax.ShapeDtypeStruct((1, 1), jnp.int32),
        ),
        in_specs=[anys] * 12,
        out_specs=(vmem, anys),
        scratch_shapes=[
            pltpu.VMEM((1, 1, seq + 2), jnp.int32), *[pltpu.VMEM((width,), BF16)] * 4,
            pltpu.SMEM((1, 1), jnp.int32),
            pltpu.VMEM((2, width, ffn), BF16),
            pltpu.VMEM((2, ffn, width), BF16),
            pltpu.VMEM((2 * width, width), BF16),
            pltpu.VMEM((width, cols - ffn), BF16),
            pltpu.VMEM((n_dp, 1, seq + 2), jnp.int32),
            pltpu.VMEM((n_dp, CAP, width), BF16),
            pltpu.VMEM((n_dp, CAP, width), BF16),
            act, act, act,
            pltpu.VMEM((seq, ffn), BF16),
            act_half, act_half,
            act,
            act_half,
            pltpu.VMEM((half, width), F32),
            act,
            pltpu.VMEM((2, 2 * half, MLP_BLOCK), F32),
            pltpu.VMEM((2 * half, LANES), F32), pltpu.VMEM((2 * half, LANES), F32), pltpu.VMEM((2 * half, LANES), F32),
            tile, pltpu.VMEM((n_pp, SUB, LANES), F32),
            tile, pltpu.VMEM((n_dp, SUB, LANES), F32),
            pltpu.VMEM((2, SUB, LANES), F32),
            dma((14,)), dma((n_dp,)), dma((n_dp,)), dma((n_dp,)), dma((n_dp,)),
            dma((n_piece,)), dma((n_piece,)), dma((n_pp,)), dma(()), dma((4, n_piece)), dma((n_piece,)), dma((n_piece,)),
            dma((n_pp,)), dma((n_pp,)), dma((2, n_dp)), dma((n_dp,)), dma((n_pp,)), dma(()), pltpu.SemaphoreType.REGULAR,
            dma((2,)), dma((2,)),
        ],
        compiler_params=pltpu.CompilerParams(collective_id=0, has_side_effects=True, vmem_limit_bytes=VMEM_LIMIT),
        name="mtp_eval",
    )(ids, *gains, emb, w1, w2, wp, u1, u2, wo)


def norm_plain(x_val):
    return norm_f32(x_val.astype(F32)).astype(BF16)


def norm_gain(x_val, gain_vec):
    return (norm_f32(x_val.astype(F32)) * gain_vec.astype(F32)).astype(BF16)


def mlp_add(x_val, normed, w_up, w_down):
    hidden = jax.nn.gelu(dot32(normed, w_up)).astype(BF16)
    return (x_val.astype(F32) + dot32(hidden, w_down)).astype(BF16)


def token_nll(normed, targets, w_out):
    n_rows, row_width = normed.shape
    n_blocks = n_rows // HEAD_ROWS

    def one_block(pair):
        block_rows, block_tgt = pair
        logits = dot32(block_rows, w_out)
        picked = jnp.take_along_axis(logits, block_tgt[:, None], axis=1)[:, 0]
        return jax.nn.logsumexp(logits, axis=1) - picked

    per_block = lax.map(one_block, (normed.reshape(n_blocks, HEAD_ROWS, row_width), targets.reshape(n_blocks, HEAD_ROWS)))
    return per_block.reshape(n_rows)


def any_ids(n_dp, n_pp, seq, ids, emb, w_one, w_two, gain_f, gain_h, gain_e, gain_m, w_proj, u_one, u_two, w_out):
    stage = lax.axis_index("pp")
    me = lax.axis_index("dp")
    n_rows, width = emb.shape
    ring = [(i, (i + 1) % n_dp) for i in range(n_dp)]
    want = ids[:seq + 1]

    def take(k, held, rows):
        local = want - lax.rem(me - k + n_dp, n_dp) * n_rows
        here = (local >= 0) & (local < n_rows)
        return jnp.where(here[:, None], held[jnp.clip(local, 0, n_rows - 1)], rows)

    def gather_step(k, carry):
        held, rows = carry
        rows = take(k, held, rows)
        return lax.ppermute(held, "dp", ring), rows

    rows = take(0, emb, jnp.zeros((seq + 1, width), BF16))
    _, rows = lax.fori_loop(1, n_dp, gather_step, (lax.ppermute(emb, "dp", ring), rows))
    to_next = [(i, i + 1) for i in range(n_pp - 1)]

    def tick(k, carry):
        x_val, _ = carry
        x_val = jnp.where((stage == 0) & (k == 0), rows[:seq], x_val)
        y_val = mlp_add(x_val, norm_plain(x_val), w_one, w_two)
        return lax.ppermute(y_val, "pp", to_next), y_val

    zero = jnp.zeros((seq, width), BF16)
    _, h_last = lax.fori_loop(0, n_pp, tick, (zero, zero))
    e_rows = lax.ppermute(rows[1:seq + 1], "pp", [(0, n_pp - 1)])
    main_nll = token_nll(norm_gain(h_last, gain_f), ids[1:seq + 1], w_out)
    z_sum = dot32(norm_gain(h_last, gain_h), w_proj[:width]) + dot32(norm_gain(e_rows, gain_e), w_proj[width:])
    z_val = z_sum.astype(BF16)
    z_val = mlp_add(z_val, norm_gain(z_val, gain_m), u_one, u_two)
    mtp_nll = token_nll(norm_gain(z_val, gain_f), ids[2:], w_out)
    is_last = stage == n_pp - 1
    main_nll = lax.psum(jnp.where(is_last, main_nll, 0.0), "pp")
    mtp_nll = lax.psum(jnp.where(is_last, mtp_nll, 0.0), "pp")
    total = lax.psum(jnp.sum(main_nll) + MTP_WEIGHT * jnp.sum(mtp_nll), "dp") / (n_dp * seq)
    return total, main_nll.reshape(1, seq), mtp_nll.reshape(1, seq)


def solution(mesh):
    n_pp = mesh.shape["pp"]
    n_dp = mesh.shape["dp"]

    def body(tok_ids, emb_s, w_one, w_two, gain_f, gain_h, gain_e, gain_m, w_proj, u_one, u_two, w_out):
        seq = tok_ids.shape[2] - 2
        gains = (gain_f, gain_h, gain_e, gain_m)
        packed, over = mega(n_dp, n_pp, seq, tok_ids, gains, emb_s, w_one, w_two, w_proj, u_one, u_two, w_out)

        def slow():
            total, main_nll, mtp_nll = any_ids(
                n_dp, n_pp, seq, tok_ids[0, 0], emb_s[0], w_one[0, 0], w_two[0, 0], *gains, w_proj, u_one, u_two, w_out)
            return total, main_nll.reshape(1, 1, seq), mtp_nll.reshape(1, 1, seq)

        def fast():
            return jnp.max(packed[2]), packed[0:1].reshape(1, 1, seq), packed[1:2].reshape(1, 1, seq)

        return lax.cond(over[0, 0] > 0, slow, fast)

    rep = P()
    in_specs = (P(None, "dp", None), P("pp", "dp", None), P("pp"), P("pp"), rep, rep, rep, rep, rep, rep, rep, rep)
    out_specs = (rep, P(None, "dp", None), P(None, "dp", None))
    return jax.shard_map(body, mesh=mesh, in_specs=in_specs, out_specs=out_specs, check_vma=False)
```

```python
import functools

import jax
import jax.numpy as jnp
from jax import lax
from jax.experimental import pallas as pl
from jax.experimental.pallas import tpu as pltpu
from jax.sharding import PartitionSpec as P

NORM_EPS = 1e-6
MTP_WEIGHT = 0.3
HEAD_ROWS = 128
LANES = 128
SUB = 8
K_TILE = 256
CAP = 24
PIECE = 512
MLP_BLOCK = 1024
E_GATE = 5
VMEM_LIMIT = 66_900_000
F32 = jnp.float32
BF16 = jnp.bfloat16
MESH = pl.DeviceIdType.MESH


def norm_f32(x_f):
    return x_f * lax.rsqrt(jnp.mean(x_f * x_f, axis=-1, keepdims=True) + NORM_EPS)


def iota(shape, dim):
    return lax.broadcasted_iota(jnp.int32, shape, dim)


def dot32(a, b):
    return jnp.dot(a, b, preferred_element_type=F32)


def shard_tiles(n_tiles, ffn):
    pair, kept = n_tiles // 2, ffn // LANES
    step = MLP_BLOCK // LANES
    even_tiles = kept + ((pair // 2 - kept) // step - 1) * step
    return even_tiles, n_tiles - pair - even_tiles


def mega_kernel(
    n_dp, n_pp, seq, cap,
    ids_hbm, gf_hbm, gh_hbm, ge_hbm, gm_hbm, emb, w1h, w2h, wph, u1h, u2h, woh,
    out_ref, flag_out,
    ids_ref, gf_ref, gh_ref, ge_ref, gm_ref, flag_buf,
    w1, w2, wp, wo,
    ids_all, picked, send_rows, recv_rows, xs, xnb, hid, ebuf, hbuf, eall, zbuf, epart, xh, lg, mx, sm, pk,
    part_send, part_recv, ls_send, ls_recv, over_buf,
    wsem, ids_ss, ids_rs, row_ss, row_rs, x_ss, x_rs, e_ss, e_rs, h_ss, h_rs, f_ss, part_ss, part_rs, ls_ss, ls_rs,
    over_ss, over_rs, link_free, push_ss, push_rs,
):
    d = lax.axis_index("dp")
    p = lax.axis_index("pp")
    width = xs.shape[2]
    ffn = w1.shape[2]
    n_rows = emb.shape[1]
    half = seq // 2
    n_shard = n_pp // 2
    shard = lax.rem(p, n_shard)
    group = p // n_shard
    n_tiles = woh.shape[1] // LANES
    even_tiles, odd_tiles = shard_tiles(n_tiles, ffn)
    tile0 = (shard // 2) * (n_tiles // 2) + lax.rem(shard, 2) * even_tiles
    cols = odd_tiles * LANES
    own_cols = wo.shape[1]
    even_cols = even_tiles * LANES - ffn
    n_piece = width // PIECE
    is_first = p == 0
    is_last = p == n_pp - 1
    even = lax.rem(p, 2) == 0
    lender = even & (p > 1)
    double = jnp.logical_not(even) & (p > 1)
    k_main = n_rows // K_TILE * K_TILE
    k_pad = k_main + K_TILE
    n_id = seq + 2
    n_slots = n_dp * cap

    col0 = pl.multiple_of(tile0 * LANES, LANES)
    tab_cp = pltpu.make_async_copy(emb.at[0], w2.at[0, pl.ds(0, n_rows), :], wsem.at[0])
    w1_cp = pltpu.make_async_copy(w1h.at[0, 0], w1.at[1], wsem.at[1])
    w2_cp = pltpu.make_async_copy(w2h.at[0, 0], w2.at[1], wsem.at[2])
    u1_cp = pltpu.make_async_copy(u1h, w1.at[0], wsem.at[3])
    u2_cp = pltpu.make_async_copy(u2h, w2.at[0], wsem.at[4])
    wp_cp = pltpu.make_async_copy(wph, wp, wsem.at[5])
    wo_even_cp = pltpu.make_async_copy(
        woh.at[:, pl.ds(col0 + ffn, even_cols)], wo.at[:, pl.ds(0, even_cols)], wsem.at[6])
    wo_odd_cp = pltpu.make_async_copy(woh.at[:, pl.ds(col0 + ffn, own_cols)], wo, wsem.at[6])
    late_cp = pltpu.make_async_copy(woh.at[:, pl.ds(col0, ffn)], w1.at[1], wsem.at[7])

    def push_copy(i):
        src, dst = ((w1h, w1), (w2h, w2))[i]
        return pltpu.make_async_remote_copy(
            src_ref=src.at[0, 0], dst_ref=dst.at[0], send_sem=push_ss.at[i], recv_sem=push_rs.at[i],
            device_id={"pp": lax.rem(p + 1, n_pp)}, device_id_type=MESH)

    small = ((ids_hbm, ids_ref), (gf_hbm, gf_ref), (gh_hbm, gh_ref), (ge_hbm, ge_ref), (gm_hbm, gm_ref))
    small_cp = [pltpu.make_async_copy(src, dst, wsem.at[8 + i]) for i, (src, dst) in enumerate(small)]
    flag_cp = pltpu.make_async_copy(flag_buf, flag_out, wsem.at[13])
    small_cp[0].start()

    barrier = pltpu.get_barrier_semaphore()
    for k in range(1, n_dp):
        pl.semaphore_signal(barrier, inc=1, device_id={"dp": lax.rem(d + k, n_dp)}, device_id_type=MESH)
    for k in range(1, n_pp):
        pl.semaphore_signal(barrier, inc=1, device_id={"pp": lax.rem(p + k, n_pp)}, device_id_type=MESH)
    @pl.when(even)
    def _():
        for k in range(1, n_dp):
            pl.semaphore_signal(
                barrier, inc=1, device_id={"dp": lax.rem(d + k, n_dp), "pp": lax.rem(p + 1, n_pp)}, device_id_type=MESH)

    for cp in small_cp[1:]:
        cp.start()

    @pl.when(is_first)
    def _():
        tab_cp.start()

    @pl.when(jnp.logical_not(even))
    def _():
        w1_cp.start()
        w2_cp.start()

    for cp in small_cp:
        cp.wait()
    pl.semaphore_wait(barrier, n_pp - 1 + jnp.where(even, 1, 2) * (n_dp - 1))

    def ids_copy(owner, peer):
        return pltpu.make_async_remote_copy(
            src_ref=ids_ref.at[0], dst_ref=ids_all.at[owner], send_sem=ids_ss.at[peer], recv_sem=ids_rs.at[owner],
            device_id={"dp": peer, "pp": 0}, device_id_type=MESH)

    @pl.when(p == 1)
    def _():
        for k in range(1, n_dp):
            ids_copy(d, lax.rem(d + k, n_dp)).start()

    @pl.when(is_first)
    def _():
        ids_all[d] = ids_ref[0]

    @pl.when(lender)
    def _():
        push_copy(0).start()
        push_copy(1).start()
        u1_cp.start()
        u2_cp.start()
        late_cp.start()

    @pl.when(p == 1)
    def _():
        u1_cp.start()
        u2_cp.start()

    @pl.when(jnp.logical_not(is_first))
    def _():
        wp_cp.start()

    @pl.when(lender)
    def _():
        wo_even_cp.start()

    @pl.when(jnp.logical_not(even))
    def _():
        wo_odd_cp.start()

    n_y = 4
    n_z = n_dp // n_y
    offs = [(z, y) for z in range(n_z) for y in range(n_y)]
    offs.sort(key=lambda o: -(min(o[0], n_z - o[0]) + min(o[1], n_y - o[1])))
    order = [lax.rem(d // n_y + z, n_z) * n_y + lax.rem(d + y, n_y) for z, y in offs]

    def row_copy(owner, j):
        return pltpu.make_async_remote_copy(
            src_ref=send_rows.at[j], dst_ref=recv_rows.at[owner], send_sem=row_ss.at[j], recv_sem=row_rs.at[owner],
            device_id={"dp": order[j]}, device_id_type=MESH)

    def positions(row0, n):
        row = ids_ref[0]
        rr = iota((n, n_id), 0) + row0
        ll = iota((n, n_id), 1)
        pos = jnp.where(rr < seq, rr, rr - seq + 1)
        id_col = jnp.sum(jnp.where(ll == pos, jnp.broadcast_to(row, (n, n_id)), 0).astype(F32), axis=1, keepdims=True)
        src_col = jnp.zeros((n, 1), F32)
        src_row = jnp.zeros((1, n_id), F32)
        for k in range(1, n_dp):
            src_col = src_col + jnp.where(id_col >= float(k * n_rows), 1.0, 0.0)
            src_row = src_row + jnp.where(row >= k * n_rows, 1.0, 0.0)
        earlier = (jnp.broadcast_to(src_row, (n, n_id)) == src_col) & (ll < pos)
        rank_col = jnp.sum(jnp.where(earlier, 1.0, 0.0), axis=1, keepdims=True)
        where_col = jnp.where(rank_col < float(cap), src_col * float(cap) + rank_col, -1.0).astype(jnp.int32)
        return jnp.where(iota((n, n_slots), 1) == where_col, 1.0, 0.0).astype(BF16)

    @pl.when(is_first)
    def _():
        xnb[:, 0:n_slots] = positions(0, seq)
        eall[:, 0:n_slots] = positions(seq, seq)
        for k in range(1, n_dp):
            peer = lax.rem(d + k, n_dp)
            ids_copy(peer, peer).wait_recv()
        w1_cp.start()
        w2_cp.start()
        low = d * n_rows
        ids2 = jnp.concatenate([ids_all[peer] for peer in order], axis=0)
        lane2 = iota((n_dp, n_id), 1)
        valid = (ids2 >= low) & (ids2 < low + n_rows) & (lane2 < seq + 1)
        before = jnp.where(iota((n_id, n_id), 0) < iota((n_id, n_id), 1), 1.0, 0.0).astype(BF16)
        rank = dot32(jnp.where(valid, 1.0, 0.0).astype(BF16), before)
        key = jnp.where(valid, rank, -1.0)
        loc = jnp.where(valid, ids2 - low, 0).astype(F32)
        picked[0] = key
        picked[1] = loc + 1.0
        slot = iota((cap, n_id), 0).astype(F32)
        tab_cp.wait()
        tail = w2[0, k_main:k_pad, :]
        w2[0, k_main:k_pad, :] = jnp.where(iota((K_TILE, width), 0) < n_rows - k_main, tail.astype(F32), 0.0).astype(BF16)
        blk = min(512, width)
        n_grp = 4

        def select(g, carry):
            row0 = pl.multiple_of(g * (n_grp * cap), 2 * SUB)
            for b in range(0, n_grp, 2):
                ids_at = []
                for s in (b, b + 1):
                    sel = picked[0, pl.ds(g * n_grp + s, 1), :] == slot
                    idx = jnp.sum(jnp.where(sel, picked[1, pl.ds(g * n_grp + s, 1), :], 0.0), axis=1, keepdims=True) - 1.0
                    ids_at.append(idx)
                idx2 = jnp.concatenate(ids_at, axis=0).astype(jnp.int32)
                hot = jnp.where(iota((2 * cap, k_pad), 1) == idx2, 1.0, 0.0).astype(BF16)
                w1[0, pl.ds(row0 + b * cap, 2 * cap), 0:k_pad] = hot
            for c in range(0, width, blk):
                got = dot32(w1[0, pl.ds(row0, n_grp * cap), 0:k_pad], w2[0, 0:k_pad, c:c + blk])
                for s in range(n_grp):
                    send_rows[g * n_grp + s, :, c:c + blk] = got[s * cap:(s + 1) * cap, :].astype(BF16)
            for at in range(n_dp // n_grp):
                @pl.when(g == at)
                def _():
                    for j in range(at * n_grp, min((at + 1) * n_grp, n_dp - 1)):
                        row_copy(d, j).start()

            return carry

        lax.fori_loop(0, n_dp // n_grp, select, 0)
        recv_rows[d] = send_rows[n_dp - 1]
        u1_cp.start()
        u2_cp.start()
        wp_cp.start()
        wo_even_cp.start()
        for j in range(n_dp - 1):
            row_copy(order[j], j).wait_recv()
        xs[1] = dot32(xnb[:, 0:n_slots], recv_rows[...].reshape(n_slots, width)).astype(BF16)

    def x_copy(i):
        part = pl.ds(i * PIECE, PIECE)
        return pltpu.make_async_remote_copy(
            src_ref=xs.at[2, :, part], dst_ref=xs.at[jnp.where(is_first, 1, 0), :, part], send_sem=x_ss.at[i], recv_sem=x_rs.at[i],
            device_id={"pp": jnp.where(is_first, 1, lax.rem(p + 2, n_pp))}, device_id_type=MESH)

    h_peers = ((3, 0), (1, 0), (5, half), (6, half))

    def h_copy(j, i):
        to, row0 = h_peers[j]
        part = pl.ds(i * PIECE, PIECE)
        return pltpu.make_async_remote_copy(
            src_ref=xs.at[2, pl.ds(row0, half), part], dst_ref=hbuf.at[:, part], send_sem=h_ss.at[j, i], recv_sem=h_rs.at[i],
            device_id={"pp": to}, device_id_type=MESH)

    def f_copy(i):
        part = pl.ds(i * PIECE, PIECE)
        return pltpu.make_async_remote_copy(
            src_ref=hbuf.at[:, part], dst_ref=hbuf.at[:, part], send_sem=f_ss.at[i], recv_sem=h_rs.at[i],
            device_id={"pp": lax.rem(p + n_pp - 1, n_pp)}, device_id_type=MESH)

    def gelu_up(m, xn, slot):
        n_blk = ffn // MLP_BLOCK
        for b in range(n_blk + 1):
            if b < n_blk:
                lg[b % 2, 0:m, :] = dot32(xn, w1[slot, :, b * MLP_BLOCK:(b + 1) * MLP_BLOCK])
            if b:
                hid[0:m, (b - 1) * MLP_BLOCK:b * MLP_BLOCK] = jax.nn.gelu(lg[(b - 1) % 2, 0:m, :]).astype(BF16)

    def stage(turn, carry):
        lent = turn == 0

        @pl.when(jnp.where(lent, double, jnp.logical_not(lender)))
        def _():
            @pl.when(lent)
            def _():
                push_copy(0).wait_recv()
                push_copy(1).wait_recv()

            @pl.when(jnp.logical_not(lent))
            def _():
                w1_cp.wait()
                w2_cp.wait()

            @pl.when(lent | (p == 1))
            def _():
                for i in range(n_piece):
                    x_copy(i).wait_recv()

            @pl.when(lent & (p == E_GATE))
            def _():
                pl.semaphore_signal(link_free, inc=1, device_id={"pp": 0}, device_id_type=MESH)

            xnb[...] = norm_f32(xs[turn].astype(F32)).astype(BF16)
            gelu_up(seq, xnb[...], turn)
            for i in range(n_piece):
                c = i * PIECE
                out = xs[turn, :, c:c + PIECE].astype(F32) + dot32(hid[...], w2[turn, :, c:c + PIECE])
                xs[turn + 1, :, c:c + PIECE] = out.astype(BF16)

                @pl.when(jnp.logical_not(lent | is_last))
                def _():
                    x_copy(i).start()

                @pl.when(jnp.logical_not(lent) & is_last)
                def _():
                    for j in range(len(h_peers)):
                        h_copy(j, i).start()

            @pl.when(lent)
            def _():
                u1_cp.start()
                u2_cp.start()

            @pl.when(jnp.logical_not(lent))
            def _():
                late_cp.start()

        return carry

    lax.fori_loop(0, 2, stage, 0)

    def e_copy(to):
        row0 = half * (to // n_shard)
        return pltpu.make_async_remote_copy(
            src_ref=eall.at[pl.ds(row0, half), :], dst_ref=ebuf, send_sem=e_ss.at[to], recv_sem=e_rs,
            device_id={"pp": to}, device_id_type=MESH)

    def over_copy(to):
        return pltpu.make_async_remote_copy(
            src_ref=over_buf.at[0], dst_ref=over_buf.at[1], send_sem=over_ss.at[to], recv_sem=over_rs,
            device_id={"pp": to}, device_id_type=MESH)

    @pl.when(is_first)
    def _():
        eall[...] = dot32(eall[:, 0:n_slots], recv_rows[...].reshape(n_slots, width)).astype(BF16)
        ids2 = ids_all[...].reshape(n_dp, n_id)
        used = iota((n_dp, n_id), 1) < seq + 1
        most = jnp.zeros((n_dp, 1), F32)
        for k in range(n_dp):
            hit = (ids2 >= k * n_rows) & (ids2 < (k + 1) * n_rows) & used
            most = jnp.maximum(most, jnp.sum(jnp.where(hit, 1.0, 0.0), axis=1, keepdims=True))
        over = jnp.broadcast_to(jnp.where(jnp.max(most, axis=0, keepdims=True) > cap, 1.0, 0.0), (SUB, LANES))
        over_buf[0] = over
        over_buf[1] = over
        ebuf[...] = eall[0:half, :]
        pl.semaphore_wait(link_free, 1)
        for to in range(1, n_pp):
            e_copy(to).start()
            over_copy(to).start()

    @pl.when(jnp.logical_not(is_first))
    def _():
        e_copy(1).wait_recv()
        over_copy(1).wait_recv()

    flag_buf[0, 0] = jnp.max(over_buf[1]).astype(jnp.int32)
    flag_cp.start()

    g_f, g_h, g_e, g_m = (ref[...].astype(F32).reshape(1, width) for ref in (gf_ref, gh_ref, ge_ref, gm_ref))

    wp_cp.wait()
    e_n = (norm_f32(ebuf[...].astype(F32)) * g_e).astype(BF16)
    epart[...] = dot32(e_n, wp[width:2 * width, :])
    u1_cp.wait()
    u2_cp.wait()

    @pl.when(even)
    def _():
        wo_even_cp.wait()

    @pl.when(jnp.logical_not(even))
    def _():
        wo_odd_cp.wait()


    row_f = jnp.broadcast_to(ids_ref[0], (2 * half, n_id))
    rr = iota((2 * half, n_id), 0)
    at = jnp.where(rr < half, rr + 1, rr - half + 2) + group * half
    tgt = jnp.sum(jnp.where(iota((2 * half, n_id), 1) == at, row_f, 0).astype(F32), axis=1, keepdims=True)
    tgt = tgt.astype(jnp.int32) - tile0 * LANES
    tgt = jnp.broadcast_to(tgt, (2 * half, LANES))

    @pl.when(is_last)
    def _():
        hbuf[...] = xs[2, half:seq, :]

    @pl.when(jnp.logical_not(is_last))
    def _():
        for i in range(n_piece):
            h_copy(0, i).wait_recv()

            @pl.when((p == 1) | (p == 3) | (p == 5))
            def _():
                f_copy(i).start()

    h_f = norm_f32(hbuf[...].astype(F32))
    z_val = (dot32((h_f * g_h).astype(BF16), wp[0:width, :]) + epart[...]).astype(BF16)
    zbuf[...] = z_val
    xh[0:half, :] = (h_f * g_f).astype(BF16)
    xnb[0:half, :] = (norm_f32(z_val.astype(F32)) * g_m).astype(BF16)
    gelu_up(half, xnb[0:half, :], 0)
    z_out = (zbuf[...].astype(F32) + dot32(hid[0:half, :], w2[0])).astype(BF16)
    xh[half:2 * half, :] = (norm_f32(z_out.astype(F32)) * g_f).astype(BF16)

    lane = iota((2 * half, LANES), 1)
    tail_ok = jnp.broadcast_to(shard == n_shard - 1, (2 * half, LANES))
    blocks = [(wo, c, ffn + c, MLP_BLOCK) for c in range(0, even_cols, MLP_BLOCK)]
    n_early = len(blocks)
    blocks += [(w1.at[1], c, c, MLP_BLOCK) for c in range(0, ffn, MLP_BLOCK)]
    n_both = len(blocks)
    blocks += [(wo, c, ffn + c, min(MLP_BLOCK, own_cols - c)) for c in range(even_cols, own_cols, MLP_BLOCK)]

    def logits_of(i):
        ref, c, _, n = blocks[i]
        lg[i % 2, :, 0:n] = dot32(xh[...], ref[:, c:c + n])

    def fold(i):
        _, _, start, n = blocks[i]
        tiles = []
        for t in range(0, n, LANES):
            val = lg[i % 2, :, t:t + LANES]
            tiles.append((start + t, val, start + t == cols - LANES))
        top = None if i == 0 else mx[...]
        for _, val, last in tiles:
            val = jnp.where(tail_ok, val, -jnp.inf) if last else val
            top = val if top is None else jnp.maximum(top, val)
        total = jnp.zeros_like(top) if i == 0 else sm[...] * jnp.exp(mx[...] - top)
        hit = jnp.zeros_like(top) if i == 0 else pk[...]
        for at_col, val, last in tiles:
            e_val = jnp.exp(val - top)
            match = lane == tgt - at_col
            if last:
                e_val = jnp.where(tail_ok, e_val, 0.0)
                match = match & tail_ok
            total = total + e_val
            hit = hit + jnp.where(match, val, 0.0)
        mx[...] = top
        sm[...] = total
        pk[...] = hit

    for i in range(n_both):
        if i == n_early:
            late_cp.wait()
        logits_of(i)
        if i:
            fold(i - 1)
    fold(n_both - 1)

    @pl.when(jnp.logical_not(even))
    def _():
        for i in range(n_both, len(blocks)):
            logits_of(i)
            if i > n_both:
                fold(i - 1)
        fold(len(blocks) - 1)

    eye = iota((2 * half, LANES), 0) == iota((2 * half, LANES), 1)

    def as_row(col):
        return jnp.sum(jnp.where(eye, jnp.broadcast_to(col, (2 * half, LANES)), 0.0), axis=0, keepdims=True)

    top = mx[...]
    m_col = jnp.max(top, axis=1, keepdims=True)
    s_col = jnp.sum(sm[...] * jnp.exp(top - m_col), axis=1, keepdims=True)
    p_col = jnp.sum(pk[...], axis=1, keepdims=True)
    sub = iota((SUB, LANES), 0)
    tile = jnp.where(sub == 0, as_row(m_col), jnp.where(sub == 1, as_row(s_col), as_row(p_col)))
    part_send[...] = tile
    part_recv[p] = tile

    def part_copy(owner, peer):
        return pltpu.make_async_remote_copy(
            src_ref=part_send, dst_ref=part_recv.at[owner], send_sem=part_ss.at[peer], recv_sem=part_rs.at[owner],
            device_id={"pp": peer}, device_id_type=MESH)

    for k in range(1, n_pp):
        part_copy(p, lax.rem(p + k, n_pp)).start()
    for k in range(1, n_pp):
        peer = lax.rem(p + k, n_pp)
        part_copy(peer, peer).wait_recv()

    def group_nll(g):
        got = [part_recv[g * n_shard + i] for i in range(n_shard)]
        best = functools.reduce(jnp.maximum, [t[0:1, :] for t in got])
        total = sum(t[1:2, :] * jnp.exp(t[0:1, :] - best) for t in got)
        return best + jnp.log(total) - sum(t[2:3, :] for t in got)

    nll_a = jnp.broadcast_to(group_nll(0), (SUB, LANES))
    nll_b = jnp.broadcast_to(group_nll(1), (SUB, LANES))
    low_lane = iota((SUB, LANES), 1) < half
    main = jnp.where(low_lane, nll_a, pltpu.roll(nll_b, half, 1))
    mtp = jnp.where(low_lane, pltpu.roll(nll_a, half, 1), nll_b)
    both = main + MTP_WEIGHT * mtp
    ls_send[...] = both
    ls_recv[d] = both

    def ls_copy(owner, peer, side):
        return pltpu.make_async_remote_copy(
            src_ref=ls_send, dst_ref=ls_recv.at[owner], send_sem=ls_ss.at[side, peer], recv_sem=ls_rs.at[owner],
            device_id={"dp": peer, "pp": lax.rem(p + n_pp - side, n_pp)}, device_id_type=MESH)

    @pl.when(jnp.logical_not(even))
    def _():
        for peer in order[:-1]:
            ls_copy(d, peer, 1).start()
            ls_copy(d, peer, 0).start()

    for peer in order[:-1]:
        ls_copy(peer, peer, 0).wait_recv()
    acc = ls_recv[0]
    for k in range(1, n_dp):
        acc = acc + ls_recv[k]
    loss = jnp.sum(acc, axis=1, keepdims=True) * (1.0 / (n_dp * seq))
    out_ref[...] = jnp.where(sub == 0, main, jnp.where(sub == 1, mtp, jnp.broadcast_to(loss, (SUB, LANES))))
    flag_cp.wait()

    @pl.when(jnp.logical_not(even))
    def _():
        for peer in order[:-1]:
            ls_copy(d, peer, 1).wait_send()
            ls_copy(d, peer, 0).wait_send()

    @pl.when(p == 1)
    def _():
        for k in range(1, n_dp):
            ids_copy(d, lax.rem(d + k, n_dp)).wait_send()

    for k in range(1, n_pp):
        part_copy(p, lax.rem(p + k, n_pp)).wait_send()

    @pl.when(is_first)
    def _():
        for k in range(1, n_dp):
            row_copy(d, k - 1).wait_send()
        for to in range(1, n_pp):
            e_copy(to).wait_send()
            over_copy(to).wait_send()

    @pl.when(jnp.logical_not(is_last | lender))
    def _():
        for i in range(n_piece):
            x_copy(i).wait_send()

    @pl.when(lender)
    def _():
        push_copy(0).wait_send()
        push_copy(1).wait_send()

    @pl.when((p == 1) | (p == 3) | (p == 5))
    def _():
        for i in range(n_piece):
            f_copy(i).wait_send()

    @pl.when(is_last)
    def _():
        for j in range(len(h_peers)):
            for i in range(n_piece):
                h_copy(j, i).wait_send()


def mega(n_dp, n_pp, seq, ids, gains, emb, w1, w2, wp, u1, u2, wo):
    width, ffn = w1.shape[2], w1.shape[3]
    cols = shard_tiles(wo.shape[1] // LANES, ffn)[1] * LANES
    half = seq // 2
    n_piece = width // PIECE
    dma = pltpu.SemaphoreType.DMA
    tile = pltpu.VMEM((SUB, LANES), F32)
    vmem = pl.BlockSpec(memory_space=pltpu.VMEM)
    anys = pl.BlockSpec(memory_space=pl.ANY)
    act = pltpu.VMEM((seq, width), BF16)
    act_half = pltpu.VMEM((half, width), BF16)
    return pl.pallas_call(
        functools.partial(mega_kernel, n_dp, n_pp, seq, CAP),
        out_shape=(
            jax.ShapeDtypeStruct((SUB, LANES), F32),
            jax.ShapeDtypeStruct((1, 1), jnp.int32),
        ),
        in_specs=[anys] * 12,
        out_specs=(vmem, anys),
        scratch_shapes=[
            pltpu.VMEM((1, 1, seq + 2), jnp.int32), *[pltpu.VMEM((width,), BF16)] * 4,
            pltpu.SMEM((1, 1), jnp.int32),
            pltpu.VMEM((2, width, ffn), BF16),
            pltpu.VMEM((2, ffn, width), BF16),
            pltpu.VMEM((2 * width, width), BF16),
            pltpu.VMEM((width, cols - ffn), BF16),
            pltpu.VMEM((n_dp, 1, seq + 2), jnp.int32),
            pltpu.VMEM((2, n_dp, seq + 2), F32),
            pltpu.VMEM((n_dp, CAP, width), BF16),
            pltpu.VMEM((n_dp, CAP, width), BF16),
            pltpu.VMEM((3, seq, width), BF16), act,
            pltpu.VMEM((seq, ffn), BF16),
            act_half, act_half,
            act,
            act_half,
            pltpu.VMEM((half, width), F32),
            act,
            pltpu.VMEM((2, 2 * half, MLP_BLOCK), F32),
            pltpu.VMEM((2 * half, LANES), F32), pltpu.VMEM((2 * half, LANES), F32), pltpu.VMEM((2 * half, LANES), F32),
            tile, pltpu.VMEM((n_pp, SUB, LANES), F32),
            tile, pltpu.VMEM((n_dp, SUB, LANES), F32),
            pltpu.VMEM((2, SUB, LANES), F32),
            dma((14,)), dma((n_dp,)), dma((n_dp,)), dma((n_dp,)), dma((n_dp,)),
            dma((n_piece,)), dma((n_piece,)), dma((n_pp,)), dma(()), dma((4, n_piece)), dma((n_piece,)), dma((n_piece,)),
            dma((n_pp,)), dma((n_pp,)), dma((2, n_dp)), dma((n_dp,)), dma((n_pp,)), dma(()), pltpu.SemaphoreType.REGULAR,
            dma((2,)), dma((2,)),
        ],
        compiler_params=pltpu.CompilerParams(collective_id=0, has_side_effects=True, vmem_limit_bytes=VMEM_LIMIT),
        name="mtp_eval",
    )(ids, *gains, emb, w1, w2, wp, u1, u2, wo)


def norm_plain(x_val):
    return norm_f32(x_val.astype(F32)).astype(BF16)


def norm_gain(x_val, gain_vec):
    return (norm_f32(x_val.astype(F32)) * gain_vec.astype(F32)).astype(BF16)


def mlp_add(x_val, normed, w_up, w_down):
    hidden = jax.nn.gelu(dot32(normed, w_up)).astype(BF16)
    return (x_val.astype(F32) + dot32(hidden, w_down)).astype(BF16)


def token_nll(normed, targets, w_out):
    n_rows, row_width = normed.shape
    n_blocks = n_rows // HEAD_ROWS

    def one_block(pair):
        block_rows, block_tgt = pair
        logits = dot32(block_rows, w_out)
        picked = jnp.take_along_axis(logits, block_tgt[:, None], axis=1)[:, 0]
        return jax.nn.logsumexp(logits, axis=1) - picked

    per_block = lax.map(one_block, (normed.reshape(n_blocks, HEAD_ROWS, row_width), targets.reshape(n_blocks, HEAD_ROWS)))
    return per_block.reshape(n_rows)


def any_ids(n_dp, n_pp, seq, ids, emb, w_one, w_two, gain_f, gain_h, gain_e, gain_m, w_proj, u_one, u_two, w_out):
    stage = lax.axis_index("pp")
    me = lax.axis_index("dp")
    n_rows, width = emb.shape
    ring = [(i, (i + 1) % n_dp) for i in range(n_dp)]
    want = ids[:seq + 1]

    def take(k, held, rows):
        local = want - lax.rem(me - k + n_dp, n_dp) * n_rows
        here = (local >= 0) & (local < n_rows)
        return jnp.where(here[:, None], held[jnp.clip(local, 0, n_rows - 1)], rows)

    def gather_step(k, carry):
        held, rows = carry
        rows = take(k, held, rows)
        return lax.ppermute(held, "dp", ring), rows

    rows = take(0, emb, jnp.zeros((seq + 1, width), BF16))
    _, rows = lax.fori_loop(1, n_dp, gather_step, (lax.ppermute(emb, "dp", ring), rows))
    to_next = [(i, i + 1) for i in range(n_pp - 1)]

    def tick(k, carry):
        x_val, _ = carry
        x_val = jnp.where((stage == 0) & (k == 0), rows[:seq], x_val)
        y_val = mlp_add(x_val, norm_plain(x_val), w_one, w_two)
        return lax.ppermute(y_val, "pp", to_next), y_val

    zero = jnp.zeros((seq, width), BF16)
    _, h_last = lax.fori_loop(0, n_pp, tick, (zero, zero))
    e_rows = lax.ppermute(rows[1:seq + 1], "pp", [(0, n_pp - 1)])
    main_nll = token_nll(norm_gain(h_last, gain_f), ids[1:seq + 1], w_out)
    z_sum = dot32(norm_gain(h_last, gain_h), w_proj[:width]) + dot32(norm_gain(e_rows, gain_e), w_proj[width:])
    z_val = z_sum.astype(BF16)
    z_val = mlp_add(z_val, norm_gain(z_val, gain_m), u_one, u_two)
    mtp_nll = token_nll(norm_gain(z_val, gain_f), ids[2:], w_out)
    is_last = stage == n_pp - 1
    main_nll = lax.psum(jnp.where(is_last, main_nll, 0.0), "pp")
    mtp_nll = lax.psum(jnp.where(is_last, mtp_nll, 0.0), "pp")
    total = lax.psum(jnp.sum(main_nll) + MTP_WEIGHT * jnp.sum(mtp_nll), "dp") / (n_dp * seq)
    return total, main_nll.reshape(1, seq), mtp_nll.reshape(1, seq)


def solution(mesh):
    n_pp = mesh.shape["pp"]
    n_dp = mesh.shape["dp"]

    def body(tok_ids, emb_s, w_one, w_two, gain_f, gain_h, gain_e, gain_m, w_proj, u_one, u_two, w_out):
        seq = tok_ids.shape[2] - 2
        gains = (gain_f, gain_h, gain_e, gain_m)
        packed, over = mega(n_dp, n_pp, seq, tok_ids, gains, emb_s, w_one, w_two, w_proj, u_one, u_two, w_out)

        def slow():
            total, main_nll, mtp_nll = any_ids(
                n_dp, n_pp, seq, tok_ids[0, 0], emb_s[0], w_one[0, 0], w_two[0, 0], *gains, w_proj, u_one, u_two, w_out)
            return total, main_nll.reshape(1, 1, seq), mtp_nll.reshape(1, 1, seq)

        def fast():
            return jnp.max(packed[2]), packed[0:1].reshape(1, 1, seq), packed[1:2].reshape(1, 1, seq)

        return lax.switch(over[0, 0], [fast, slow])

    rep = P()
    in_specs = (P(None, "dp", None), P("pp", "dp", None), P("pp"), P("pp"), rep, rep, rep, rep, rep, rep, rep, rep)
    out_specs = (rep, P(None, "dp", None), P(None, "dp", None))
    return jax.shard_map(body, mesh=mesh, in_specs=in_specs, out_specs=out_specs, check_vma=False)
```
